32 devices in a mesh: grp: 2 (over y), blk: 8 (over z, x), cross: 2 (over core).
Axes of the slice: x: 2, y: 2, z: 4, core: 2. Of those that a mesh axis runs over, the one named last changes fastest.
Arguments:
- orbitals: bfloat16 [32, 40, 1600], P(('grp', 'blk', 'cross')), parts along dimension 0, may hold values from -6 to 6
- response: bfloat16 [32, 40, 1600], P(('grp', 'blk', 'cross')), parts along dimension 0, may hold values from -6 to 6
- pair_mask: int32 [32, 4], P(('grp', 'blk', 'cross')), parts along dimension 0, may hold values 0 or 1
Outputs:
- tangent_exchange: bfloat16 [32, 40, 1600], P(('grp', 'blk', 'cross')), parts along dimension 0
The draws below stay inside these ranges and needn't reach their ends.
There are 2 independent parts, one for each index of `grp`. The reference program is written for one: setup_inputs(seed, part) draws one part's arguments, and reference() takes and returns one part's arrays. A program takes and returns all parts, laid end to end along the dimension named above; each array names one. Nothing has to cross between parts.
All inputs are finite; a program needn't handle non-finite values. No bound on the sum of `pair_mask` on one device may be relied on, other than what follows from the above.
Results may differ from the reference program's by a relative error of at most 0.017.
Values may be sent and summed in bfloat16 or wider, within the bound.
No kernel may reach another device: no remote copies, remote signals or barrier semaphores. Data moves between devices by JAX's collectives and lax.ppermute only.
A program may use at most 64 MiB of HBM per device.

```python
import jax
import jax.numpy as jnp
from jax import lax

NG = 40
ORBS = 16


def with_ends(result, stream_key, least, high):
    place = [jax.random.randint(jax.random.fold_in(stream_key, axis), (), 0, length) for axis, length in enumerate(result.shape)]
    longest = result.shape.index(max(result.shape))
    neighbour = place[:longest] + [(place[longest] + 1) % result.shape[longest]] + place[longest + 1:]
    return result.at[tuple(place)].set(least).at[tuple(neighbour)].set(high)


def block_levels(own_key, dims, pieces, low, top_value):
    gain, own = 1.0, jax.random.fold_in(own_key, 6)
    for axis_at, parts in pieces:
        draws = jnp.exp(jax.random.uniform(jax.random.fold_in(own, axis_at), (parts,), jnp.float32, low / len(pieces), top_value / len(pieces)))
        gain = gain * jnp.repeat(draws, dims[axis_at] // parts).reshape([-1 if axis == axis_at else 1 for axis in range(len(dims))])
    return gain


def centred(stream_key, dims, scale, bound, split=(), held_as=jnp.bfloat16):
    drawn = scale * jax.random.normal(stream_key, dims, jnp.float32)
    if split:
        drawn = drawn * block_levels(stream_key, dims, split, -0.22, 0.18)
    return jnp.clip(drawn, -bound, bound).astype(held_as)


def setup_inputs(seed: int = 0, part: int = 0) -> dict:
    key_of = jax.random.split(jax.random.key(seed), 4)
    own_keys = jax.random.split(jax.random.fold_in(key_of[3], part), 4)
    return {
        "orbitals": centred(own_keys[0], (ORBS, NG, NG * NG), 1.0, 6.0, ((0, 16),)),
        "response": centred(own_keys[1], (ORBS, NG, NG * NG), 1.0, 6.0, ((0, 16),)),
        "pair_mask": with_ends((jax.random.randint(own_keys[2], (ORBS, 4), 0, 4) < 3).astype(jnp.int32), jax.random.fold_in(own_keys[2], 1), 0, 1),
    }


mixing = 0.25

def dft_tables(length):
    positions = jnp.arange(length, dtype=jnp.int32)
    phases = positions[:, None] * positions[None, :] % length
    angles = phases.astype(jnp.float32) * (2.0 * jnp.pi / length)
    scaling = 1.0 / jnp.sqrt(jnp.float32(length))
    cosine = (jnp.cos(angles) * scaling).astype(jnp.bfloat16)
    sines = (jnp.sin(angles) * scaling).astype(jnp.bfloat16)
    forward = jnp.concatenate([jnp.concatenate([cosine, sines], 1), jnp.concatenate([-sines, cosine], 1)], 0)
    inverse = jnp.concatenate([jnp.concatenate([cosine, -sines], 1), jnp.concatenate([sines, cosine], 1)], 0)
    return (forward, inverse)

def coulomb(length):
    positions = jnp.arange(length, dtype=jnp.int32)
    frequency = jnp.where(positions <= length // 2, positions, positions - length).astype(jnp.float32)
    squares = frequency * frequency
    norm_squared = squares[:, None, None] + squares[None, :, None] + squares[None, None, :]
    values = 1.0 / (0.0625 + 25.0 * norm_squared / (length * length))
    values = jnp.where(norm_squared > 0.5, values, jnp.float32(0.0))
    return values.reshape(length, length * length)

def apply_section(matrix, stacked):
    length = stacked.shape[0] // 2
    product = jnp.dot(matrix, stacked, preferred_element_type=jnp.float32).astype(jnp.bfloat16)
    volume = product.reshape(2, length, length, length)
    return jnp.transpose(volume, (0, 2, 3, 1)).reshape(2 * length, length * length)

def potentials(own_orbital, own_response, far_orbital, far_response, forward, inverse, kernel):
    length = own_orbital.shape[0]
    own_f = own_orbital.astype(jnp.float32)
    far_f = far_orbital.astype(jnp.float32)
    ground = (own_f * far_f).astype(jnp.bfloat16)
    tangent = (own_response.astype(jnp.float32) * far_f + own_f * far_response.astype(jnp.float32)).astype(jnp.bfloat16)
    spectrum = jnp.concatenate([ground, tangent], 0)
    for repeat in range(3):
        spectrum = apply_section(forward, spectrum)
    filtered = (spectrum.reshape(2, length, -1).astype(jnp.float32) * kernel[None]).astype(jnp.bfloat16)
    filtered = filtered.reshape(2 * length, -1)
    for repeat in range(3):
        filtered = apply_section(inverse, filtered)
    return (filtered[:length], filtered[length:])

def contribution(partner, partner_response, ground, tangent):
    return (partner_response.astype(jnp.float32) * ground.astype(jnp.float32) + partner.astype(jnp.float32) * tangent.astype(jnp.float32)).astype(jnp.bfloat16)

def reference(orbitals, response, pair_mask):
    forward, inverse = dft_tables(NG)
    kernel = coulomb(NG)

    def both_terms(items):
        own_orbital, own_response, far_orbital, far_response = items
        ground, tangent = potentials(own_orbital, own_response, far_orbital, far_response, forward, inverse, kernel)
        return (contribution(far_orbital, far_response, ground, tangent), contribution(own_orbital, own_response, ground, tangent))
    self_term = lax.map(lambda items: both_terms((items[0], items[1], items[0], items[1]))[0], (orbitals, response))
    later_orbital = jnp.roll(orbitals, -2, 0)
    later_response = jnp.roll(response, -2, 0)
    later_term, handed = lax.map(both_terms, (orbitals, response, later_orbital, later_response))
    prior_term = jnp.roll(handed, 2, 0)
    even_term, odd_term = lax.map(both_terms, (orbitals[0::2], response[0::2], orbitals[1::2], response[1::2]))
    mate_term = jnp.stack([even_term, odd_term], 1).reshape(orbitals.shape)
    weights = pair_mask.astype(jnp.float32)
    total = weights[:, 0, None, None] * self_term.astype(jnp.float32) + weights[:, 1, None, None] * mate_term.astype(jnp.float32) + weights[:, 2, None, None] * prior_term.astype(jnp.float32) + weights[:, 3, None, None] * later_term.astype(jnp.float32)
    return (-mixing * total).astype(jnp.bfloat16)
```

```python
import functools

import jax
import jax.numpy as jnp
import numpy as np
from jax import lax
from jax.experimental import pallas as pl
from jax.experimental.pallas import tpu as pltpu
from jax.sharding import PartitionSpec as P

mixing = 0.25
chunk = 256
bf16 = jnp.bfloat16
f32 = jnp.float32


def from_partner(value, axis, bit):
    mask = 2**bit
    pairs = [(source, source ^ mask) for source in range(lax.axis_size(axis))]
    return lax.ppermute(value, axis, pairs)


def shifted(value, axis, by):
    devices = lax.axis_size(axis)
    return lax.ppermute(value, axis, [(i, (i + by) % devices) for i in range(devices)])


def real_table(length):
    positions = np.arange(length)
    angles = (positions[:, None] * positions[None, :] % length) * (2.0 * np.pi / length)
    return ((np.cos(angles) + np.sin(angles)) / np.sqrt(length)).astype(np.float32)


def coulomb(length):
    positions = np.arange(length)
    frequency = np.where(positions <= length // 2, positions, positions - length)
    squares = (frequency * frequency).astype(np.float64)
    norm = squares[:, None, None] + squares[None, :, None] + squares[None, None, :]
    values = np.where(norm > 0.5, 1.0 / (0.0625 + 25.0 * norm / (length * length)), 0.0)
    return values.reshape(length, length * length).astype(np.float32)


def spans(total):
    return [(at, min(chunk, total - at)) for at in range(0, total, chunk)]


def products(own, own_r, far, far_r):
    return [own * far, own_r * far + own * far_r]


def filtered(fields, table, blocks, kernel, mid):
    rows, total = fields.shape
    count = rows // kernel.shape[0]
    for at, size in spans(total):
        part = jnp.dot(fields[...], table[:, at : at + size], preferred_element_type=f32)
        part = jnp.dot(blocks[...], part.astype(bf16), preferred_element_type=f32)
        gains = jnp.concatenate([kernel[:, at : at + size]] * count, 0)
        part = jnp.dot(blocks[...], (part * gains).astype(bf16), preferred_element_type=f32)
        mid[:, at : at + size] = part.astype(bf16)


def near_body(mask, own, own_r, mate, mate_r, wide, tall, blocks, kernel, table, total, fields, mid):
    length, area = own.shape
    for y in range(0, length, 2):
        for at, size in spans(area):
            cols = slice(at, at + size)
            upper = wide[y : y + 1, cols] * tall[:, cols]
            lower = wide[y + 1 : y + 2, cols] * tall[:, cols]
            table[y * length : (y + 2) * length, cols] = jnp.concatenate([upper, lower], 0).astype(bf16)
    for at, size in spans(area):
        cols = slice(at, at + size)
        o, r = own[:, cols].astype(f32), own_r[:, cols].astype(f32)
        m, s = mate[:, cols].astype(f32), mate_r[:, cols].astype(f32)
        fields[:, cols] = jnp.concatenate(products(o, r, o, r) + products(o, r, m, s), 0).astype(bf16)
    filtered(fields, table, blocks, kernel, mid)
    first, second = mask[0, 0].astype(f32), mask[0, 1].astype(f32)
    for at, size in spans(area):
        cols = slice(at, at + size)
        part = jnp.dot(mid[...], table[:, cols], preferred_element_type=f32)
        o, r = own[:, cols].astype(f32), own_r[:, cols].astype(f32)
        m, s = mate[:, cols].astype(f32), mate_r[:, cols].astype(f32)
        a, b = part[:length], part[length : 2 * length]
        c, d = part[2 * length : 3 * length], part[3 * length :]
        total[:, cols] = first * (r * a + o * b) + second * (s * c + m * d)


def far_body(mask, own, own_r, far, far_r, blocks, kernel, table, near, handed, total, fields, mid):
    length, area = own.shape
    for at, size in spans(area):
        cols = slice(at, at + size)
        o, r = own[:, cols].astype(f32), own_r[:, cols].astype(f32)
        m, s = far[:, cols].astype(f32), far_r[:, cols].astype(f32)
        fields[:, cols] = jnp.concatenate(products(o, r, m, s), 0).astype(bf16)
    filtered(fields, table, blocks, kernel, mid)
    third = mask[0, 2].astype(f32)
    for at, size in spans(area):
        cols = slice(at, at + size)
        part = jnp.dot(mid[...], table[:, cols], preferred_element_type=f32)
        o, r = own[:, cols].astype(f32), own_r[:, cols].astype(f32)
        m, s = far[:, cols].astype(f32), far_r[:, cols].astype(f32)
        a, b = part[:length], part[length:]
        handed[:, cols] = (r * a + o * b).astype(bf16)
        total[:, cols] = near[:, cols] + third * (s * a + m * b)


vmem = pl.BlockSpec(memory_space=pltpu.VMEM)
smem = pl.BlockSpec(memory_space=pltpu.SMEM)


def run(body, operands, outs, rows, area, limit):
    return pl.pallas_call(
        body,
        out_shape=outs,
        in_specs=[smem] + [vmem] * (len(operands) - 1),
        out_specs=[vmem] * len(outs),
        scratch_shapes=[pltpu.VMEM((rows, area), bf16), pltpu.VMEM((rows, area), bf16)],
        compiler_params=pltpu.CompilerParams(vmem_limit_bytes=limit),
        cost_estimate=pl.CostEstimate(flops=4 * rows * area * area, bytes_accessed=rows * area * 8, transcendentals=0),
    )(*operands)


def shards(orbitals, response, pair_mask):
    own, own_r = orbitals[0], response[0]
    length, area = own.shape
    base = real_table(length)
    wide = jnp.asarray(np.repeat(base, length, axis=1))
    tall = jnp.asarray(np.tile(base, (1, length)))
    kernel = jnp.asarray(coulomb(length))
    four = jnp.asarray(np.kron(np.eye(4), base).astype(np.float32)).astype(bf16)
    two = jnp.asarray(np.kron(np.eye(2), base).astype(np.float32)).astype(bf16)
    mate, mate_r = from_partner((own, own_r), "cross", 0)
    far, far_r = shifted((own, own_r), "blk", 1)
    table, near = run(
        near_body,
        (pair_mask, own, own_r, mate, mate_r, wide, tall, four, kernel),
        [jax.ShapeDtypeStruct((area, area), bf16), jax.ShapeDtypeStruct((length, area), f32)],
        4 * length,
        area,
        24 << 20,
    )
    handed, total = run(
        far_body,
        (pair_mask, own, own_r, far, far_r, two, kernel, table, near),
        [jax.ShapeDtypeStruct((length, area), bf16), jax.ShapeDtypeStruct((length, area), f32)],
        2 * length,
        area,
        24 << 20,
    )
    later = shifted(handed, "blk", -1)
    last = pair_mask[0, 3].astype(f32)
    return (-mixing * (total + last * later.astype(f32))).astype(bf16)[None]


def solution(mesh):
    spec = P(("grp", "blk", "cross"), None, None)
    return jax.shard_map(
        shards,
        mesh=mesh,
        in_specs=(spec, spec, P(("grp", "blk", "cross"), None)),
        out_specs=spec,
        check_vma=False,
    )
```

```python
import functools

import jax
import jax.numpy as jnp
import numpy as np
from jax import lax
from jax.experimental import pallas as pl
from jax.experimental.pallas import tpu as pltpu
from jax.sharding import PartitionSpec as P

mixing = 0.25
lane = 128
bf16 = jnp.bfloat16
f32 = jnp.float32


def from_partner(value, axis, bit):
    mask = 2**bit
    pairs = [(source, source ^ mask) for source in range(lax.axis_size(axis))]
    return lax.ppermute(value, axis, pairs)


def shifted(value, axis, by):
    devices = lax.axis_size(axis)
    return lax.ppermute(value, axis, [(i, (i + by) % devices) for i in range(devices)])


def real_table(length):
    positions = np.arange(length)
    angles = (positions[:, None] * positions[None, :] % length) * (2.0 * np.pi / length)
    return ((np.cos(angles) + np.sin(angles)) / np.sqrt(length)).astype(np.float32)


def coulomb(length):
    positions = np.arange(length)
    frequency = np.where(positions <= length // 2, positions, positions - length)
    squares = (frequency * frequency).astype(np.float64)
    norm = squares[:, None, None] + squares[None, :, None] + squares[None, None, :]
    values = np.where(norm > 0.5, 1.0 / (0.0625 + 25.0 * norm / (length * length)), 0.0)
    return values.reshape(length, length * length).astype(np.float32)


def slabs(total):
    return [(at, min(lane, total - at)) for at in range(0, total, lane)]


def products(own, own_r, far, far_r):
    return [own * far, own_r * far + own * far_r]


def joined(ref, first, count):
    return jnp.concatenate([ref[first + step] for step in range(count)], 1)


def pairs(total):
    count = len(slabs(total))
    return [(at, min(2, count - at)) for at in range(0, count, 2)]


def through(values, table, spots):
    area = table.shape[1]
    totals = [None] * len(spots)
    for first, size in pairs(area):
        depth = min(size * lane, area - first * lane)
        left = joined(values, first, size)[:, :depth]
        for which, (at, count) in enumerate(spots):
            right = jnp.concatenate(
                [table[at + step, first * lane : first * lane + depth, :] for step in range(count)], 1
            )
            part = jnp.dot(left, right, preferred_element_type=f32)
            totals[which] = part if totals[which] is None else totals[which] + part
    return totals


def twos(items):
    return [items[at : at + 2] for at in range(0, len(items), 2)]


def filtered(fields, table, blocks, kernel, mid):
    area = table.shape[1]
    length = kernel.shape[0]
    copies = fields.shape[1] // length

    def across(spots, parts):
        parts = [jnp.dot(blocks[...], part.astype(bf16), preferred_element_type=f32) for part in parts]
        for which, (at, count) in enumerate(spots):
            width = min(count * lane, area - at * lane)
            gains = kernel[:, at * lane : at * lane + width]
            if width < count * lane:
                gains = jnp.concatenate([gains, jnp.zeros((length, count * lane - width), f32)], 1)
            parts[which] = (parts[which] * jnp.concatenate([gains] * copies, 0)).astype(bf16)
        parts = [jnp.dot(blocks[...], part, preferred_element_type=f32) for part in parts]
        for (at, count), part in zip(spots, parts):
            for step in range(count):
                mid[at + step] = part[:, step * lane : (step + 1) * lane].astype(bf16)

    waiting = None
    for spots in twos(pairs(area)):
        parts = through(fields, table, spots)
        if waiting is not None:
            across(*waiting)
        waiting = (spots, parts)
    across(*waiting)


def put(ref, slab, value):
    width = value.shape[1]
    if width < lane:
        value = jnp.concatenate([value, jnp.zeros((value.shape[0], lane - width), value.dtype)], 1)
    ref[slab] = value.astype(bf16)


def outcomes(mid, table):
    area = table.shape[1]
    for spots in twos(pairs(area)):
        for spot, part in zip(spots, through(mid, table, spots)):
            yield spot, part[:, : min(spot[1] * lane, area - spot[0] * lane)]


def near_body(
    mask_in, own_in, own_r_in, mate, mate_r, wide_in, tall_in, kernel_in, blocks_in,
    table, near, own, own_r, kernel,
    mask, wide, tall, blocks, fields, mid, sems,
):
    length, area = own.shape
    moves = [
        pltpu.make_async_copy(source, target, sems.at[at])
        for at, (source, target) in enumerate(
            [
                (wide_in, wide), (tall_in, tall), (own_in, own), (own_r_in, own_r),
                (blocks_in, blocks),
                (kernel_in, kernel), (mask_in, mask),
            ]
        )
    ]
    for move in moves:
        move.start()
    moves[0].wait()
    moves[1].wait()
    for slab, (at, size) in enumerate(slabs(area)):
        cols = slice(at, at + size)
        low = tall[:, cols]
        for y in range(0, length, 2):
            value = jnp.concatenate([wide[y : y + 1, cols] * low, wide[y + 1 : y + 2, cols] * low], 0)
            if size < lane:
                value = jnp.concatenate([value, jnp.zeros((2 * length, lane - size), f32)], 1)
            table[slab, y * length : (y + 2) * length, :] = value.astype(bf16)
    for move in moves[2:]:
        move.wait()
    for slab, (at, size) in enumerate(slabs(area)):
        cols = slice(at, at + size)
        o, r = own[:, cols].astype(f32), own_r[:, cols].astype(f32)
        m, s = mate[:, cols].astype(f32), mate_r[:, cols].astype(f32)
        put(fields, slab, jnp.concatenate(products(o, r, o, r) + products(o, r, m, s), 0))
    filtered(fields, table, blocks, kernel, mid)
    first, second = mask[0, 0].astype(f32), mask[0, 1].astype(f32)
    for spot, part in outcomes(mid, table):
        at, width = spot[0], part.shape[1]
        cols = slice(at * lane, at * lane + width)
        o, r = own[:, cols].astype(f32), own_r[:, cols].astype(f32)
        m, s = mate[:, cols].astype(f32), mate_r[:, cols].astype(f32)
        a, b = part[:length], part[length : 2 * length]
        c, d = part[2 * length : 3 * length], part[3 * length :]
        near[:, cols] = first * (r * a + o * b) + second * (s * c + m * d)


def far_body(mask, own, own_r, far, far_r, blocks, kernel, table, near, handed, total, fields, mid):
    length, area = own.shape
    for slab, (at, size) in enumerate(slabs(area)):
        cols = slice(at, at + size)
        o, r = own[:, cols].astype(f32), own_r[:, cols].astype(f32)
        m, s = far[:, cols].astype(f32), far_r[:, cols].astype(f32)
        put(fields, slab, jnp.concatenate(products(o, r, m, s), 0))
    filtered(fields, table, blocks, kernel, mid)
    third = mask[0, 2].astype(f32)
    for spot, part in outcomes(mid, table):
        at, width = spot[0], part.shape[1]
        cols = slice(at * lane, at * lane + width)
        o, r = own[:, cols].astype(f32), own_r[:, cols].astype(f32)
        m, s = far[:, cols].astype(f32), far_r[:, cols].astype(f32)
        a, b = part[:length], part[length:]
        handed[:, cols] = (r * a + o * b).astype(bf16)
        total[:, cols] = near[:, cols] + third * (s * a + m * b)


vmem = pl.BlockSpec(memory_space=pltpu.VMEM)
smem = pl.BlockSpec(memory_space=pltpu.SMEM)
hbm = pl.BlockSpec(memory_space=pltpu.HBM)


def cost(rows, area):
    return pl.CostEstimate(flops=4 * rows * area * area, bytes_accessed=rows * area * 8, transcendentals=0)


def shards(orbitals, response, pair_mask):
    own, own_r = orbitals[0], response[0]
    length, area = own.shape
    count = len(slabs(area))
    base = real_table(length)
    wide = jnp.asarray(np.repeat(base, length, axis=1))
    tall = jnp.asarray(np.tile(base, (1, length)))
    kernel = jnp.asarray(coulomb(length))
    four = jnp.asarray(np.kron(np.eye(4), base).astype(np.float32)).astype(bf16)
    two = jnp.asarray(np.kron(np.eye(2), base).astype(np.float32)).astype(bf16)
    mate, mate_r = from_partner((own, own_r), "cross", 0)
    far, far_r = shifted((own, own_r), "blk", 1)
    plane = lambda kind: jax.ShapeDtypeStruct((length, area), kind)
    held = lambda kind: pltpu.VMEM((length, area), kind)
    table, near, own_held, own_r_held, kernel_held = pl.pallas_call(
        near_body,
        out_shape=[jax.ShapeDtypeStruct((count, area, lane), bf16), plane(f32), plane(bf16), plane(bf16), plane(f32)],
        in_specs=[hbm] * 3 + [vmem] * 2 + [hbm] * 4,
        out_specs=[vmem] * 5,
        scratch_shapes=[
            pltpu.SMEM(pair_mask.shape, jnp.int32), held(f32), held(f32),
            pltpu.VMEM(four.shape, bf16),
            pltpu.VMEM((count, 4 * length, lane), bf16),
            pltpu.VMEM((count, 4 * length, lane), bf16),
            pltpu.SemaphoreType.DMA((7,)),
        ],
        compiler_params=pltpu.CompilerParams(vmem_limit_bytes=24 << 20),
        cost_estimate=cost(4 * length, area),
    )(*(pltpu.with_memory_space_constraint(value, pltpu.HBM) for value in (pair_mask, own, own_r)), mate, mate_r, *(pltpu.with_memory_space_constraint(value, pltpu.HBM) for value in (wide, tall, kernel, four)))
    handed, total = pl.pallas_call(
        far_body,
        out_shape=[plane(bf16), plane(f32)],
        in_specs=[smem] + [vmem] * 8,
        out_specs=[vmem] * 2,
        scratch_shapes=[pltpu.VMEM((count, 2 * length, lane), bf16)] * 2,
        compiler_params=pltpu.CompilerParams(vmem_limit_bytes=16 << 20),
        cost_estimate=cost(2 * length, area),
    )(pair_mask, own_held, own_r_held, far, far_r, two, kernel_held, table, near)
    later = shifted(handed, "blk", -1)
    last = pair_mask[0, 3].astype(f32)
    return (-mixing * (total + last * later.astype(f32))).astype(bf16)[None]


def solution(mesh):
    spec = P(("grp", "blk", "cross"), None, None)
    return jax.shard_map(
        shards,
        mesh=mesh,
        in_specs=(spec, spec, P(("grp", "blk", "cross"), None)),
        out_specs=spec,
        check_vma=False,
    )
```

```python
import jax
import jax.numpy as jnp
import numpy as np
from jax import lax
from jax.experimental import pallas as pl
from jax.experimental.pallas import tpu as pltpu
from jax.sharding import PartitionSpec as P


mixing = 0.25
lane = 128
bf16 = jnp.bfloat16
f32 = jnp.float32


def from_partner(value, axis, bit):
    mask = 2**bit
    pairs = [(source, source ^ mask) for source in range(lax.axis_size(axis))]
    return lax.ppermute(value, axis, pairs)


def shifted(value, axis, by):
    devices = lax.axis_size(axis)
    return lax.ppermute(value, axis, [(i, (i + by) % devices) for i in range(devices)])


def real_table(length):
    positions = np.arange(length)
    angles = (positions[:, None] * positions[None, :] % length) * (2.0 * np.pi / length)
    return ((np.cos(angles) + np.sin(angles)) / np.sqrt(length)).astype(np.float32)


def coulomb(length):
    positions = np.arange(length)
    frequency = np.where(positions <= length // 2, positions, positions - length)
    squares = (frequency * frequency).astype(np.float64)
    norm = squares[:, None, None] + squares[None, :, None] + squares[None, None, :]
    values = np.where(norm > 0.5, 1.0 / (0.0625 + 25.0 * norm / (length * length)), 0.0)
    return values.reshape(length, length * length).astype(np.float32)


def slabs(total):
    return [(at, min(lane, total - at)) for at in range(0, total, lane)]


def products(own, own_r, far, far_r):
    return [own * far, own_r * far + own * far_r]


def joined(ref, first, count):
    return jnp.concatenate([ref[first + step] for step in range(count)], 1)


def pairs(total):
    count = len(slabs(total))
    return [(at, min(2, count - at)) for at in range(0, count, 2)]


def through(values, table, spots):
    area = table.shape[1]
    totals = [None] * len(spots)
    for first, size in pairs(area):
        depth = min(size * lane, area - first * lane)
        left = joined(values, first, size)[:, :depth]
        for which, (at, count) in enumerate(spots):
            right = jnp.concatenate(
                [table[at + step, first * lane : first * lane + depth, :] for step in range(count)], 1
            )
            part = jnp.dot(left, right, preferred_element_type=f32)
            totals[which] = part if totals[which] is None else totals[which] + part
    return totals


def twos(items):
    return [items[at : at + 2] for at in range(0, len(items), 2)]


def filtered(fields, table, blocks, kernel, mid):
    area = table.shape[1]
    length = kernel.shape[0]
    copies = fields.shape[1] // length

    def across(spots, parts):
        parts = [jnp.dot(blocks[...], part.astype(bf16), preferred_element_type=f32) for part in parts]
        for which, (at, count) in enumerate(spots):
            width = min(count * lane, area - at * lane)
            gains = kernel[:, at * lane : at * lane + width]
            if width < count * lane:
                gains = jnp.concatenate([gains, jnp.zeros((length, count * lane - width), f32)], 1)
            parts[which] = (parts[which] * jnp.concatenate([gains] * copies, 0)).astype(bf16)
        parts = [jnp.dot(blocks[...], part, preferred_element_type=f32) for part in parts]
        for (at, count), part in zip(spots, parts):
            for step in range(count):
                mid[at + step] = part[:, step * lane : (step + 1) * lane].astype(bf16)

    waiting = None
    for spots in twos(pairs(area)):
        parts = through(fields, table, spots)
        if waiting is not None:
            across(*waiting)
        waiting = (spots, parts)
    across(*waiting)


def put(ref, slab, value):
    width = value.shape[1]
    if width < lane:
        value = jnp.concatenate([value, jnp.zeros((value.shape[0], lane - width), value.dtype)], 1)
    ref[slab] = value.astype(bf16)


def outcomes(mid, table):
    area = table.shape[1]
    for spots in twos(pairs(area)):
        for spot, part in zip(spots, through(mid, table, spots)):
            yield spot, part[:, : min(spot[1] * lane, area - spot[0] * lane)]


def self_body(
    own_in, own_r_in, wide_in, tall_in, kernel_in, blocks_in, mask_in,
    table, near, own, own_r, kernel, blocks, shares,
    mask, wide, tall, fields, mid, sems,
):
    length, area = own.shape
    moves = [
        pltpu.make_async_copy(source, target, sems.at[at])
        for at, (source, target) in enumerate(
            [
                (wide_in, wide), (tall_in, tall), (own_in, own), (own_r_in, own_r),
                (kernel_in, kernel), (blocks_in, blocks), (mask_in, mask),
            ]
        )
    ]
    for move in moves:
        move.start()
    moves[0].wait()
    moves[1].wait()
    for slab, (at, size) in enumerate(slabs(area)):
        cols = slice(at, at + size)
        low = tall[:, cols]
        for y in range(0, length, 2):
            value = jnp.concatenate([wide[y : y + 1, cols] * low, wide[y + 1 : y + 2, cols] * low], 0)
            if size < lane:
                value = jnp.concatenate([value, jnp.zeros((2 * length, lane - size), f32)], 1)
            table[slab, y * length : (y + 2) * length, :] = value.astype(bf16)
    for move in moves[2:]:
        move.wait()
    for at in range(shares.shape[0]):
        weight = -mixing * mask[0, at].astype(f32)
        shares[at : at + 1, :] = jnp.full((1, area), weight, f32)
    for cols, (o, r, a, b) in responses(own, own_r, own, own_r, blocks, kernel, table, fields, mid):
        near[:, cols] = r * a + o * b


def responses(own, own_r, far, far_r, blocks, kernel, table, fields, mid):
    length, area = own.shape
    for slab, (at, size) in enumerate(slabs(area)):
        cols = slice(at, at + size)
        o, r = own[:, cols].astype(f32), own_r[:, cols].astype(f32)
        m, s = far[:, cols].astype(f32), far_r[:, cols].astype(f32)
        put(fields, slab, jnp.concatenate(products(o, r, m, s), 0))
    filtered(fields, table, blocks, kernel, mid)
    for spot, part in outcomes(mid, table):
        at, width = spot[0], part.shape[1]
        cols = slice(at * lane, at * lane + width)
        yield cols, (far[:, cols].astype(f32), far_r[:, cols].astype(f32), part[:length], part[length:])


def far_body(own, own_r, far, far_r, blocks, kernel, table, handed, prior, fields, mid):
    for cols, (m, s, a, b) in responses(own, own_r, far, far_r, blocks, kernel, table, fields, mid):
        o, r = own[:, cols].astype(f32), own_r[:, cols].astype(f32)
        handed[:, cols] = (r * a + o * b).astype(bf16)
        prior[:, cols] = s * a + m * b


def mate_body(own, own_r, mate, mate_r, blocks, kernel, table, near, prior, shares, total, fields, mid):
    for cols, (m, s, a, b) in responses(own, own_r, mate, mate_r, blocks, kernel, table, fields, mid):
        first, second, third = (shares[at : at + 1, cols] for at in range(3))
        total[:, cols] = first * near[:, cols] + second * (s * a + m * b) + third * prior[:, cols]


vmem = pl.BlockSpec(memory_space=pltpu.VMEM)
hbm = pl.BlockSpec(memory_space=pltpu.HBM)


def cost(rows, area):
    return pl.CostEstimate(flops=4 * rows * area * area, bytes_accessed=rows * area * 8, transcendentals=0)


def shards(orbitals, response, pair_mask):
    own, own_r = orbitals[0], response[0]
    length, area = own.shape
    count = len(slabs(area))
    base = real_table(length)
    wide = jnp.asarray(np.repeat(base, length, axis=1))
    tall = jnp.asarray(np.tile(base, (1, length)))
    kernel = jnp.asarray(coulomb(length))
    blocks = jnp.asarray(np.kron(np.eye(2), base).astype(np.float32)).astype(bf16)
    far, far_r = shifted((own, own_r), "blk", 1)
    mate, mate_r = from_partner((own, own_r), "cross", 0)
    plane = lambda kind: jax.ShapeDtypeStruct((length, area), kind)
    held = lambda kind: pltpu.VMEM((length, area), kind)
    inner = [pltpu.VMEM((count, 2 * length, lane), bf16)] * 2
    fixed = lambda value: pltpu.with_memory_space_constraint(value, pltpu.HBM)
    table, near, own_held, own_r_held, kernel_held, blocks_held, shares = pl.pallas_call(
        self_body,
        out_shape=[
            jax.ShapeDtypeStruct((count, area, lane), bf16), plane(f32), plane(bf16), plane(bf16), plane(f32),
            jax.ShapeDtypeStruct(blocks.shape, bf16), jax.ShapeDtypeStruct((pair_mask.shape[1], area), f32),
        ],
        in_specs=[hbm] * 7,
        out_specs=[vmem] * 7,
        scratch_shapes=[pltpu.SMEM(pair_mask.shape, jnp.int32), held(f32), held(f32), *inner, pltpu.SemaphoreType.DMA((7,))],
        compiler_params=pltpu.CompilerParams(vmem_limit_bytes=24 << 20),
        cost_estimate=cost(4 * length, area),
    )(*(fixed(value) for value in (own, own_r, wide, tall, kernel, blocks, pair_mask)))
    shared = (blocks_held, kernel_held, table)
    handed, prior = pl.pallas_call(
        far_body,
        out_shape=[plane(bf16), plane(f32)],
        in_specs=[vmem] * 7,
        out_specs=[vmem] * 2,
        scratch_shapes=inner,
        compiler_params=pltpu.CompilerParams(vmem_limit_bytes=16 << 20),
        cost_estimate=cost(2 * length, area),
    )(own_held, own_r_held, far, far_r, *shared)
    later = shifted(handed, "blk", -1)
    total = pl.pallas_call(
        mate_body,
        out_shape=plane(f32),
        in_specs=[vmem] * 10,
        out_specs=vmem,
        scratch_shapes=inner,
        compiler_params=pltpu.CompilerParams(vmem_limit_bytes=16 << 20),
        cost_estimate=cost(2 * length, area),
    )(own_held, own_r_held, mate, mate_r, *shared, near, prior, shares)
    return (total + shares[3:] * later.astype(f32)).astype(bf16)[None]


def solution(mesh):
    spec = P(("grp", "blk", "cross"), None, None)
    return jax.shard_map(
        shards,
        mesh=mesh,
        in_specs=(spec, spec, P(("grp", "blk", "cross"), None)),
        out_specs=spec,
        check_vma=False,
    )
```

```python
import jax
import jax.numpy as jnp
import numpy as np
from jax import lax
from jax.experimental import pallas as pl
from jax.experimental.pallas import tpu as pltpu
from jax.sharding import PartitionSpec as P


mixing = 0.25
lane = 128
bf16 = jnp.bfloat16
f32 = jnp.float32


def from_partner(value, axis, bit):
    mask = 2**bit
    pairs = [(source, source ^ mask) for source in range(lax.axis_size(axis))]
    return lax.ppermute(value, axis, pairs)


def shifted(value, axis, by):
    devices = lax.axis_size(axis)
    return lax.ppermute(value, axis, [(i, (i + by) % devices) for i in range(devices)])


def real_table(length):
    positions = np.arange(length)
    angles = (positions[:, None] * positions[None, :] % length) * (2.0 * np.pi / length)
    return (np.cos(angles) + np.sin(angles)) / np.sqrt(length)


def half_tables(length):
    half = length // 2 + 1
    positions = np.arange(half)
    angles = (positions[:, None] * positions[None, :] % length) * (2.0 * np.pi / length)
    twice = np.where((positions == 0) | (2 * positions == length), 1.0, 2.0)[:, None]
    return twice * np.cos(angles) / np.sqrt(length), twice * np.sin(angles) * (twice > 1.5) / np.sqrt(length)


def coulomb(length):
    positions = np.arange(length)
    frequency = np.where(positions <= length // 2, positions, positions - length)
    squares = (frequency * frequency).astype(np.float64)
    norm = squares[:, None, None] + squares[None, :, None] + squares[None, None, :]
    values = np.where(norm > 0.5, 1.0 / (0.0625 + 25.0 * norm / (length * length)), 0.0)
    return values.reshape(length, length * length)


def slab_count(width):
    return -(-width // lane)


def filled(values):
    return np.pad(values, ((0, 0), (0, slab_count(values.shape[1]) * lane - values.shape[1]))).astype(np.float32)


def twos(count):
    return [(at, min(2, count - at)) for at in range(0, count, 2)]


def mirrored(source, slab, length, limit):
    area = length * length
    column = lax.broadcasted_iota(jnp.int32, (length, lane), 1)
    result = None
    at, stop = slab * lane, min((slab + 1) * lane, limit)
    while at < stop:
        y = at // length
        delta = area - 2 * length * y if y else 0
        origin = (at + delta) // lane
        end = min(stop, (y + 1) * length, (origin + 1) * lane - delta)
        piece = source(origin)
        turn = -delta % lane
        if turn:
            piece = pltpu.roll(piece, turn, 1)
        result = piece if result is None else jnp.where(column >= at - slab * lane, piece, result)
        at = end
    return result


def natural(ref):
    area = ref.shape[1]
    kept = {}

    def slab(at):
        if at not in kept:
            value = ref[:, at * lane : min((at + 1) * lane, area)].astype(f32)
            if value.shape[1] < lane:
                value = jnp.concatenate([value, jnp.zeros((value.shape[0], lane - value.shape[1]), f32)], 1)
            kept[at] = value
        return kept[at]

    return slab


def split(ref, parts):
    count = parts.shape[0] // 2
    length = ref.shape[0]
    source = natural(ref)
    for at in range(count):
        there = mirrored(source, at, length, (length // 2 + 1) * length)
        parts[at] = 0.5 * (source(at) + there)
        parts[count + at] = 0.5 * (source(at) - there)


def products(left, right):
    return left[0] * right[0] + left[1] * right[1], left[0] * right[1] + left[1] * right[0]


def both(ref, at):
    count = ref.shape[0] // 2
    return ref[at], ref[count + at]


def summed(left, right):
    return left[0] + right[0], left[1] + right[1]


def through(values, table, spots):
    count, depth = table.shape[0] // 2, table.shape[1]
    totals = [None] * len(spots)
    for first, size in twos(count):
        low, high = first * lane, min((first + size) * lane, depth)
        for which, (parity, at, width) in enumerate(spots):
            base = parity * count
            left = jnp.concatenate([values[base + first + step] for step in range(size)], 1)[:, : high - low]
            right = jnp.concatenate([table[base + at + step, low:high, :] for step in range(width)], 1)
            part = jnp.dot(left, right, preferred_element_type=f32)
            totals[which] = part if totals[which] is None else totals[which] + part
    return totals


def pair(own, own_r, far, far_r, blocks, kernel, table, fields, mid):
    count, length = kernel.shape[0], kernel.shape[1]
    for at in range(count):
        ground = products(both(own, at), both(far, at))
        tangent = summed(products(both(own_r, at), both(far, at)), products(both(own, at), both(far_r, at)))
        for parity in range(2):
            fields[parity * count + at] = jnp.concatenate([ground[parity], tangent[parity]], 0).astype(bf16)

    def across(spots, parts):
        parts = [jnp.dot(blocks[...], part.astype(bf16), preferred_element_type=f32) for part in parts]
        for which, (parity, at, width) in enumerate(spots):
            gains = jnp.concatenate([kernel[at + step] for step in range(width)], 1)
            parts[which] = (parts[which] * jnp.concatenate([gains] * 2, 0)).astype(bf16)
        parts = [jnp.dot(blocks[...], part, preferred_element_type=f32) for part in parts]
        for (parity, at, width), part in zip(spots, parts):
            for step in range(width):
                mid[parity * count + at + step] = part[:, step * lane : (step + 1) * lane].astype(bf16)

    waiting = None
    for at, width in twos(count):
        spots = [(0, at, width), (1, at, width)]
        parts = through(fields, table, spots)
        if waiting is not None:
            across(*waiting)
        waiting = (spots, parts)
    across(*waiting)
    for at, width in twos(count):
        even, odd = through(mid, table, [(0, at, width), (1, at, width)])
        for step in range(width):
            cols = slice(step * lane, (step + 1) * lane)
            yield at + step, (even[:length, cols], odd[:length, cols]), (even[length:, cols], odd[length:, cols])


def term(partner, partner_r, at, ground, tangent):
    return summed(products(both(partner_r, at), ground), products(both(partner, at), tangent))


def whole(results, length, put):
    area, limit = length * length, (length // 2 + 1) * length
    column = lax.broadcasted_iota(jnp.int32, (length, lane), 1)
    count = slab_count(limit)
    for at in range(slab_count(area)):
        value = None
        if at < count:
            value = results[at][0] + results[at][1]
        if (at + 1) * lane > limit:
            there = mirrored_from(results, at, length, limit, area)
            value = there if value is None else jnp.where(column < limit - at * lane, value, there)
        put(at, value)


def mirrored_from(results, slab, length, limit, area):
    column = lax.broadcasted_iota(jnp.int32, (length, lane), 1)
    result = None
    at, stop = max(slab * lane, limit), min((slab + 1) * lane, area)
    while at < stop:
        y = at // length
        delta = area - 2 * length * y
        origin = (at + delta) // lane
        end = min(stop, (y + 1) * length, (origin + 1) * lane - delta)
        piece = results[origin][0] - results[origin][1]
        turn = -delta % lane
        if turn:
            piece = pltpu.roll(piece, turn, 1)
        result = piece if result is None else jnp.where(column >= at - slab * lane, piece, result)
        at = end
    return result


def store(ref):
    area = ref.shape[1]

    def put(at, value):
        width = min(lane, area - at * lane)
        ref[:, at * lane : at * lane + width] = value[:, :width].astype(ref.dtype)

    return put


def self_body(
    own_in, own_r_in, wide_in, tall_in, kernel_in, blocks_in, mask_in,
    table, near, own, own_r, kernel, blocks, shares,
    mask, wide, tall, plain, plain_r, fields, mid, sems,
):
    length = plain.shape[0]
    half = length // 2 + 1
    count = kernel.shape[0]
    moves = [
        pltpu.make_async_copy(source, target, sems.at[at])
        for at, (source, target) in enumerate(
            [
                (wide_in, wide), (tall_in, tall), (own_in, plain), (own_r_in, plain_r),
                (kernel_in, kernel), (blocks_in, blocks), (mask_in, mask),
            ]
        )
    ]
    for move in moves:
        move.start()
    moves[0].wait()
    moves[1].wait()
    for parity in range(2):
        for at in range(count):
            cols = slice(at * lane, (at + 1) * lane)
            low = tall[:, cols]
            for y in range(0, half, 2):
                rows = [wide[parity, row : row + 1, cols] * low for row in range(y, min(y + 2, half))]
                value = jnp.concatenate(rows, 0)
                table[parity * count + at, y * length : y * length + value.shape[0], :] = value.astype(bf16)
    for move in moves[2:]:
        move.wait()
    for at in range(shares.shape[0]):
        weight = -mixing * mask[0, at].astype(f32)
        shares[at : at + 1, :] = jnp.full((1, shares.shape[1]), weight, f32)
    split(plain, own)
    split(plain_r, own_r)
    for at, ground, tangent in pair(own, own_r, own, own_r, blocks, kernel, table, fields, mid):
        near[at], near[count + at] = term(own, own_r, at, ground, tangent)


def far_body(own, own_r, plain, plain_r, blocks, kernel, table, handed, prior, far, far_r, fields, mid):
    count = kernel.shape[0]
    split(plain, far)
    split(plain_r, far_r)
    results = []
    for at, ground, tangent in pair(own, own_r, far, far_r, blocks, kernel, table, fields, mid):
        results.append(term(own, own_r, at, ground, tangent))
        prior[at], prior[count + at] = term(far, far_r, at, ground, tangent)
    whole(results, plain.shape[0], store(handed))


def mate_body(own, own_r, plain, plain_r, blocks, kernel, table, near, prior, shares, total, far, far_r, fields, mid):
    split(plain, far)
    split(plain_r, far_r)
    first, second, third = (shares[at : at + 1, :lane] for at in range(3))
    results = []
    for at, ground, tangent in pair(own, own_r, far, far_r, blocks, kernel, table, fields, mid):
        parts = zip(both(near, at), term(far, far_r, at, ground, tangent), both(prior, at))
        results.append(tuple(first * a + second * b + third * c for a, b, c in parts))
    whole(results, plain.shape[0], store(total))


vmem = pl.BlockSpec(memory_space=pltpu.VMEM)
hbm = pl.BlockSpec(memory_space=pltpu.HBM)


def cost(rows, area):
    return pl.CostEstimate(flops=2 * rows * area * area, bytes_accessed=rows * area * 8, transcendentals=0)


def shards(orbitals, response, pair_mask):
    own, own_r = orbitals[0], response[0]
    length, area = own.shape
    folded = (length // 2 + 1) * length
    count = slab_count(folded)
    base = real_table(length)
    wide = np.stack([filled(np.repeat(part, length, axis=1)) for part in half_tables(length)])
    tall = filled(np.tile(base, (1, length // 2 + 1)))
    kernel = filled(coulomb(length)[:, :folded]).reshape(length, count, lane).transpose(1, 0, 2)
    blocks = jnp.asarray(np.kron(np.eye(2), base).astype(np.float32)).astype(bf16)
    far, far_r = shifted((own, own_r), "blk", 1)
    mate, mate_r = from_partner((own, own_r), "cross", 0)
    plane = lambda kind: jax.ShapeDtypeStruct((length, area), kind)
    parts = jax.ShapeDtypeStruct((2 * count, length, lane), f32)
    held = pltpu.VMEM((2 * count, length, lane), f32)
    inner = [pltpu.VMEM((2 * count, 2 * length, lane), bf16)] * 2
    fixed = lambda value: pltpu.with_memory_space_constraint(jnp.asarray(value), pltpu.HBM)
    table, near, own_parts, own_r_parts, kernel_held, blocks_held, shares = pl.pallas_call(
        self_body,
        out_shape=[
            jax.ShapeDtypeStruct((2 * count, folded, lane), bf16), parts, parts, parts,
            jax.ShapeDtypeStruct(kernel.shape, f32), jax.ShapeDtypeStruct(blocks.shape, bf16),
            jax.ShapeDtypeStruct((pair_mask.shape[1], area), f32),
        ],
        in_specs=[hbm] * 7,
        out_specs=[vmem] * 7,
        scratch_shapes=[
            pltpu.SMEM(pair_mask.shape, jnp.int32), pltpu.VMEM(wide.shape, f32), pltpu.VMEM(tall.shape, f32),
            pltpu.VMEM((length, area), bf16), pltpu.VMEM((length, area), bf16), *inner,
            pltpu.SemaphoreType.DMA((7,)),
        ],
        compiler_params=pltpu.CompilerParams(vmem_limit_bytes=24 << 20),
        cost_estimate=cost(4 * length, area),
    )(*(fixed(value) for value in (own, own_r, wide, tall, kernel, blocks, pair_mask)))
    shared = (blocks_held, kernel_held, table)
    handed, prior = pl.pallas_call(
        far_body,
        out_shape=[plane(bf16), parts],
        in_specs=[vmem] * 7,
        out_specs=[vmem] * 2,
        scratch_shapes=[held, held, *inner],
        compiler_params=pltpu.CompilerParams(vmem_limit_bytes=16 << 20),
        cost_estimate=cost(2 * length, area),
    )(own_parts, own_r_parts, far, far_r, *shared)
    later = shifted(handed, "blk", -1)
    total = pl.pallas_call(
        mate_body,
        out_shape=plane(f32),
        in_specs=[vmem] * 10,
        out_specs=vmem,
        scratch_shapes=[held, held, *inner],
        compiler_params=pltpu.CompilerParams(vmem_limit_bytes=16 << 20),
        cost_estimate=cost(2 * length, area),
    )(own_parts, own_r_parts, mate, mate_r, *shared, near, prior, shares)
    return (total + shares[3:] * later.astype(f32)).astype(bf16)[None]


def solution(mesh):
    spec = P(("grp", "blk", "cross"), None, None)
    return jax.shard_map(
        shards,
        mesh=mesh,
        in_specs=(spec, spec, P(("grp", "blk", "cross"), None)),
        out_specs=spec,
        check_vma=False,
    )
```

```python
import jax
import jax.numpy as jnp
import numpy as np
from jax import lax
from jax.experimental import pallas as pl
from jax.experimental.pallas import tpu as pltpu
from jax.sharding import PartitionSpec as P


mixing = 0.25
lane = 128
bf16 = jnp.bfloat16
f32 = jnp.float32


def from_partner(value, axis, bit):
    mask = 2**bit
    pairs = [(source, source ^ mask) for source in range(lax.axis_size(axis))]
    return lax.ppermute(value, axis, pairs)


def shifted(value, axis, by):
    devices = lax.axis_size(axis)
    return lax.ppermute(value, axis, [(i, (i + by) % devices) for i in range(devices)])


def real_table(length):
    positions = np.arange(length)
    angles = (positions[:, None] * positions[None, :] % length) * (2.0 * np.pi / length)
    return (np.cos(angles) + np.sin(angles)) / np.sqrt(length)


def half_tables(length):
    half = length // 2 + 1
    positions = np.arange(half)
    angles = (positions[:, None] * positions[None, :] % length) * (2.0 * np.pi / length)
    twice = np.where((positions == 0) | (2 * positions == length), 1.0, 2.0)[:, None]
    return twice * np.cos(angles) / np.sqrt(length), twice * np.sin(angles) * (twice > 1.5) / np.sqrt(length)


def coulomb(length):
    positions = np.arange(length)
    frequency = np.where(positions <= length // 2, positions, positions - length)
    squares = (frequency * frequency).astype(np.float64)
    norm = squares[:, None, None] + squares[None, :, None] + squares[None, None, :]
    values = np.where(norm > 0.5, 1.0 / (0.0625 + 25.0 * norm / (length * length)), 0.0)
    return values.reshape(length, length * length)


def slab_count(width):
    return -(-width // lane)


def filled(values):
    return np.pad(values, ((0, 0), (0, slab_count(values.shape[1]) * lane - values.shape[1]))).astype(np.float32)


def twos(count):
    return [(at, min(2, count - at)) for at in range(0, count, 2)]


def mirrored(source, slab, length, limit, base=0):
    area = length * length
    column = lax.broadcasted_iota(jnp.int32, (length, lane), 1)
    result = None
    at, stop = max(slab * lane, base), min((slab + 1) * lane, limit)
    while at < stop:
        y = at // length
        delta = area - 2 * length * y if y else 0
        origin = (at + delta) // lane
        end = min(stop, (y + 1) * length, (origin + 1) * lane - delta)
        piece = source(origin)
        turn = -delta % lane
        if turn:
            piece = pltpu.roll(piece, turn, 1)
        result = piece if result is None else jnp.where(column >= at - slab * lane, piece, result)
        at = end
    return result


def natural(ref):
    area = ref.shape[1]
    kept = {}

    def slab(at):
        if at not in kept:
            value = ref[:, at * lane : min((at + 1) * lane, area)].astype(f32)
            if value.shape[1] < lane:
                value = jnp.concatenate([value, jnp.zeros((value.shape[0], lane - value.shape[1]), f32)], 1)
            kept[at] = value
        return kept[at]

    return slab


def split(ref, parts):
    count = parts.shape[0] // 2
    length = ref.shape[0]
    source = natural(ref)
    for at in range(count):
        there = mirrored(source, at, length, (length // 2 + 1) * length)
        parts[at] = 0.5 * (source(at) + there)
        parts[count + at] = 0.5 * (source(at) - there)


def products(left, right):
    return left[0] * right[0] + left[1] * right[1], left[0] * right[1] + left[1] * right[0]


def both(ref, at):
    count = ref.shape[0] // 2
    return ref[at], ref[count + at]


def summed(left, right):
    return left[0] + right[0], left[1] + right[1]


def through(values, table, spots, totals, firsts):
    count, depth = table.shape[0] // 2, table.shape[1]
    totals = totals or [None] * len(spots)
    for first, size in firsts:
        low, high = first * lane, min((first + size) * lane, depth)
        for which, (parity, at, width) in enumerate(spots):
            base = parity * count
            left = jnp.concatenate([values[base + first + step] for step in range(size)], 1)[:, : high - low]
            right = jnp.concatenate([table[base + at + step, low:high, :] for step in range(width)], 1)
            part = jnp.dot(left, right, preferred_element_type=f32)
            totals[which] = part if totals[which] is None else totals[which] + part
    return totals


def pair(own, own_r, far, far_r, blocks, kernel, table, fields, mid):
    count, length = kernel.shape[0], kernel.shape[1]
    tiles = twos(count)
    for at in range(count):
        ground = products(both(own, at), both(far, at))
        tangent = summed(products(both(own_r, at), both(far, at)), products(both(own, at), both(far_r, at)))
        for parity in range(2):
            fields[parity * count + at] = jnp.concatenate([ground[parity], tangent[parity]], 0).astype(bf16)

    def across(spots, parts):
        parts = [jnp.dot(blocks[...], part.astype(bf16), preferred_element_type=f32) for part in parts]
        for which, (parity, at, width) in enumerate(spots):
            gains = jnp.concatenate([kernel[at + step] for step in range(width)], 1)
            parts[which] = (parts[which] * jnp.concatenate([gains] * 2, 0)).astype(bf16)
        parts = [jnp.dot(blocks[...], part, preferred_element_type=f32) for part in parts]
        for (parity, at, width), part in zip(spots, parts):
            for step in range(width):
                mid[parity * count + at + step] = part[:, step * lane : (step + 1) * lane].astype(bf16)

    spots = [[(parity, at, width) for parity in range(2)] for at, width in tiles]
    parts = [through(fields, table, spot, None, tiles) for spot in spots]
    across(sum(spots, []), sum(parts, []))
    for spot in spots:
        even, odd = through(mid, table, spot, None, tiles)
        for step in range(spot[0][2]):
            cols = slice(step * lane, (step + 1) * lane)
            yield spot[0][1] + step, (even[:length, cols], odd[:length, cols]), (even[length:, cols], odd[length:, cols])


def term(partner, partner_r, at, ground, tangent):
    return summed(products(both(partner_r, at), ground), products(both(partner, at), tangent))


def whole(results, length, put):
    area, limit = length * length, (length // 2 + 1) * length
    column = lax.broadcasted_iota(jnp.int32, (length, lane), 1)
    count, stop = slab_count(limit), slab_count(area)
    lowest = stop
    direct, apart = [], []
    for at, parts in enumerate(results):
        direct.append(parts[0] + parts[1])
        apart.append(parts[0] - parts[1])
        if (at + 1) * lane <= limit:
            put(at, direct[at])
        while lowest > limit // lane and needed(lowest - 1, length, limit) <= at:
            lowest -= 1
            there = mirrored(lambda slab: apart[slab], lowest, length, area, limit)
            if lowest < count:
                there = jnp.where(column < limit - lowest * lane, direct[lowest], there)
            put(lowest, there)


def needed(slab, length, limit):
    y = max(slab * lane, limit) // length
    return max((max(slab * lane, limit) + length * length - 2 * length * y + length - 1) // lane, slab if slab * lane < limit else 0)


def store(ref):
    area = ref.shape[1]

    def put(at, value):
        width = min(lane, area - at * lane)
        ref[:, at * lane : at * lane + width] = value[:, :width].astype(ref.dtype)

    return put


def self_body(
    own_in, own_r_in, wide_in, tall_in, kernel_in, blocks_in, mask_in,
    table, near, own, own_r, kernel, blocks, shares,
    mask, wide, tall, plain, plain_r, fields, mid, sems,
):
    length = plain.shape[0]
    half = length // 2 + 1
    count = kernel.shape[0]
    moves = [
        pltpu.make_async_copy(source, target, sems.at[at])
        for at, (source, target) in enumerate(
            [
                (wide_in, wide), (tall_in, tall), (own_in, plain), (own_r_in, plain_r),
                (kernel_in, kernel), (blocks_in, blocks), (mask_in, mask),
            ]
        )
    ]
    for move in moves:
        move.start()
    moves[0].wait()
    moves[1].wait()
    for parity in range(2):
        for at in range(count):
            cols = slice(at * lane, (at + 1) * lane)
            low = tall[:, cols]
            for y in range(0, half, 2):
                rows = [wide[parity, row : row + 1, cols] * low for row in range(y, min(y + 2, half))]
                value = jnp.concatenate(rows, 0)
                table[parity * count + at, y * length : y * length + value.shape[0], :] = value.astype(bf16)
    for move in moves[2:]:
        move.wait()
    for at in range(shares.shape[0]):
        weight = -mixing * mask[0, at].astype(f32)
        shares[at : at + 1, :] = jnp.full((1, shares.shape[1]), weight, f32)
    split(plain, own)
    split(plain_r, own_r)
    for at, ground, tangent in pair(own, own_r, own, own_r, blocks, kernel, table, fields, mid):
        near[at], near[count + at] = term(own, own_r, at, ground, tangent)


def far_body(own, own_r, far, plain_r, blocks, kernel, table, handed, prior, far_r, fields, mid):
    count = kernel.shape[0]
    split(plain_r, far_r)

    def results():
        for at, ground, tangent in pair(own, own_r, far, far_r, blocks, kernel, table, fields, mid):
            yield term(own, own_r, at, ground, tangent)
            prior[at], prior[count + at] = term(far, far_r, at, ground, tangent)

    whole(results(), plain_r.shape[0], store(handed))


def mate_body(own, own_r, plain, plain_r, blocks, kernel, table, near, prior, shares, total, far, far_r, fields, mid):
    split(plain, far)
    split(plain_r, far_r)
    first, second, third = (shares[at : at + 1, :lane] for at in range(3))

    def results():
        for at, ground, tangent in pair(own, own_r, far, far_r, blocks, kernel, table, fields, mid):
            parts = zip(both(near, at), term(far, far_r, at, ground, tangent), both(prior, at))
            yield tuple(first * a + second * b + third * c for a, b, c in parts)

    whole(results(), plain.shape[0], store(total))


vmem = pl.BlockSpec(memory_space=pltpu.VMEM)
hbm = pl.BlockSpec(memory_space=pltpu.HBM)


def cost(rows, area):
    return pl.CostEstimate(flops=2 * rows * area * area, bytes_accessed=rows * area * 8, transcendentals=0)


def shards(orbitals, response, pair_mask):
    own, own_r = orbitals[0], response[0]
    length, area = own.shape
    folded = (length // 2 + 1) * length
    count = slab_count(folded)
    base = real_table(length)
    wide = np.stack([filled(np.repeat(part, length, axis=1)) for part in half_tables(length)])
    tall = filled(np.tile(base, (1, length // 2 + 1)))
    kernel = filled(coulomb(length)[:, :folded]).reshape(length, count, lane).transpose(1, 0, 2)
    blocks = jnp.asarray(np.kron(np.eye(2), base).astype(np.float32)).astype(bf16)
    far, far_r = shifted((own, own_r), "blk", 1)
    mate, mate_r = from_partner((own, own_r), "cross", 0)
    plane = lambda kind: jax.ShapeDtypeStruct((length, area), kind)
    parts = jax.ShapeDtypeStruct((2 * count, length, lane), f32)
    held = pltpu.VMEM((2 * count, length, lane), f32)
    inner = [pltpu.VMEM((2 * count, 2 * length, lane), bf16)] * 2
    fixed = lambda value: pltpu.with_memory_space_constraint(jnp.asarray(value), pltpu.HBM)
    table, near, own_parts, own_r_parts, kernel_held, blocks_held, shares = pl.pallas_call(
        self_body,
        out_shape=[
            jax.ShapeDtypeStruct((2 * count, folded, lane), bf16), parts, parts, parts,
            jax.ShapeDtypeStruct(kernel.shape, f32), jax.ShapeDtypeStruct(blocks.shape, bf16),
            jax.ShapeDtypeStruct((pair_mask.shape[1], area), f32),
        ],
        in_specs=[hbm] * 7,
        out_specs=[vmem] * 7,
        scratch_shapes=[
            pltpu.SMEM(pair_mask.shape, jnp.int32), pltpu.VMEM(wide.shape, f32), pltpu.VMEM(tall.shape, f32),
            pltpu.VMEM((length, area), bf16), pltpu.VMEM((length, area), bf16), *inner,
            pltpu.SemaphoreType.DMA((7,)),
        ],
        compiler_params=pltpu.CompilerParams(vmem_limit_bytes=24 << 20),
        cost_estimate=cost(4 * length, area),
    )(*(fixed(value) for value in (own, own_r, wide, tall, kernel, blocks, pair_mask)))
    shared = (blocks_held, kernel_held, table)
    far_parts = pl.pallas_call(
        split,
        out_shape=parts,
        in_specs=[vmem],
        out_specs=vmem,
        compiler_params=pltpu.CompilerParams(vmem_limit_bytes=8 << 20),
        cost_estimate=cost(2, area),
    )(far)
    handed, prior = pl.pallas_call(
        far_body,
        out_shape=[plane(bf16), parts],
        in_specs=[vmem] * 7,
        out_specs=[vmem] * 2,
        scratch_shapes=[held, *inner],
        compiler_params=pltpu.CompilerParams(vmem_limit_bytes=16 << 20),
        cost_estimate=cost(2 * length, area),
    )(own_parts, own_r_parts, far_parts, far_r, *shared)
    later = shifted(handed, "blk", -1)
    total = pl.pallas_call(
        mate_body,
        out_shape=plane(f32),
        in_specs=[vmem] * 10,
        out_specs=vmem,
        scratch_shapes=[held, held, *inner],
        compiler_params=pltpu.CompilerParams(vmem_limit_bytes=16 << 20),
        cost_estimate=cost(2 * length, area),
    )(own_parts, own_r_parts, mate, mate_r, *shared, near, prior, shares)
    return (total + shares[3:] * later.astype(f32)).astype(bf16)[None]


def solution(mesh):
    spec = P(("grp", "blk", "cross"), None, None)
    return jax.shard_map(
        shards,
        mesh=mesh,
        in_specs=(spec, spec, P(("grp", "blk", "cross"), None)),
        out_specs=spec,
        check_vma=False,
    )
```

```python
import jax
import jax.numpy as jnp
import numpy as np
from jax import lax
from jax.experimental import pallas as pl
from jax.experimental.pallas import tpu as pltpu
from jax.sharding import PartitionSpec as P


mixing = 0.25
lane = 128
bf16 = jnp.bfloat16
f32 = jnp.float32


def from_partner(value, axis, bit):
    mask = 2**bit
    pairs = [(source, source ^ mask) for source in range(lax.axis_size(axis))]
    return lax.ppermute(value, axis, pairs)


def shifted(value, axis, by):
    devices = lax.axis_size(axis)
    return lax.ppermute(value, axis, [(i, (i + by) % devices) for i in range(devices)])


def real_table(length):
    positions = np.arange(length)
    angles = (positions[:, None] * positions[None, :] % length) * (2.0 * np.pi / length)
    return (np.cos(angles) + np.sin(angles)) / np.sqrt(length)


def half_tables(length):
    half = length // 2 + 1
    positions = np.arange(half)
    angles = (positions[:, None] * positions[None, :] % length) * (2.0 * np.pi / length)
    twice = np.where((positions == 0) | (2 * positions == length), 1.0, 2.0)[:, None]
    return twice * np.cos(angles) / np.sqrt(length), twice * np.sin(angles) * (twice > 1.5) / np.sqrt(length)


def coulomb(length):
    positions = np.arange(length)
    frequency = np.where(positions <= length // 2, positions, positions - length)
    squares = (frequency * frequency).astype(np.float64)
    norm = squares[:, None, None] + squares[None, :, None] + squares[None, None, :]
    values = np.where(norm > 0.5, 1.0 / (0.0625 + 25.0 * norm / (length * length)), 0.0)
    return values.reshape(length, length * length)


def slab_count(width):
    return -(-width // lane)


def filled(values):
    return np.pad(values, ((0, 0), (0, slab_count(values.shape[1]) * lane - values.shape[1]))).astype(np.float32)


def twos(count):
    return [(at, min(2, count - at)) for at in range(0, count, 2)]


def mirrored(source, slab, length, limit, base=0):
    area = length * length
    column = lax.broadcasted_iota(jnp.int32, (length, lane), 1)
    result = None
    at, stop = max(slab * lane, base), min((slab + 1) * lane, limit)
    while at < stop:
        y = at // length
        delta = area - 2 * length * y if y else 0
        origin = (at + delta) // lane
        end = min(stop, (y + 1) * length, (origin + 1) * lane - delta)
        piece = source(origin)
        turn = -delta % lane
        if turn:
            piece = pltpu.roll(piece, turn, 1)
        result = piece if result is None else jnp.where(column >= at - slab * lane, piece, result)
        at = end
    return result


def natural(ref):
    area = ref.shape[1]
    kept = {}

    def slab(at):
        if at not in kept:
            value = ref[:, at * lane : min((at + 1) * lane, area)].astype(f32)
            if value.shape[1] < lane:
                value = jnp.concatenate([value, jnp.zeros((value.shape[0], lane - value.shape[1]), f32)], 1)
            kept[at] = value
        return kept[at]

    return slab


def halves(source, at, length):
    there = mirrored(source, at, length, (length // 2 + 1) * length)
    return 0.5 * (source(at) + there), 0.5 * (source(at) - there)


def split(ref, parts):
    source = natural(ref)
    for at in range(parts.shape[0] // 2):
        keep(parts, at, halves(source, at, ref.shape[0]))


def keep(ref, at, parts):
    count = ref.shape[0] // 2
    ref[at], ref[count + at] = parts


def products(left, right):
    return left[0] * right[0] + left[1] * right[1], left[0] * right[1] + left[1] * right[0]


def both(ref, at):
    count = ref.shape[0] // 2
    return ref[at], ref[count + at]


def summed(left, right):
    return left[0] + right[0], left[1] + right[1]


def through(values, table, spots, firsts):
    count, depth = table.shape[0] // 2, table.shape[1]
    totals = [None] * len(spots)
    for first, size in firsts:
        low, high = first * lane, min((first + size) * lane, depth)
        for which, (parity, at, width) in enumerate(spots):
            base = parity * count
            left = jnp.concatenate([values[base + first + step] for step in range(size)], 1)[:, : high - low]
            right = jnp.concatenate([table[base + at + step, low:high, :] for step in range(width)], 1)
            part = jnp.dot(left, right, preferred_element_type=f32)
            totals[which] = part if totals[which] is None else totals[which] + part
    return totals


def convolved(fields, blocks, kernel, table, mid):
    count, length = kernel.shape[0], kernel.shape[1]
    rows = fields.shape[1]
    tiles = twos(count)
    spots = [[(parity, at, width) for parity in range(2)] for at, width in tiles]
    parts = sum([through(fields, table, spot, tiles) for spot in spots], [])
    step_matrix = blocks[:rows, :rows]
    parts = [jnp.dot(step_matrix, part.astype(bf16), preferred_element_type=f32) for part in parts]
    for which, (parity, at, width) in enumerate(sum(spots, [])):
        gains = jnp.concatenate([kernel[at + step] for step in range(width)], 1)
        parts[which] = (parts[which] * jnp.concatenate([gains] * (rows // length), 0)).astype(bf16)
    parts = [jnp.dot(step_matrix, part, preferred_element_type=f32) for part in parts]
    for (parity, at, width), part in zip(sum(spots, []), parts):
        for step in range(width):
            mid[parity * count + at + step] = part[:, step * lane : (step + 1) * lane].astype(bf16)
    for spot in spots:
        even, odd = through(mid, table, spot, tiles)
        for step in range(spot[0][2]):
            cols = slice(step * lane, (step + 1) * lane)
            yield spot[0][1] + step, even[:, cols], odd[:, cols]


def pair(own, own_r, far, far_r, blocks, kernel, table, fields, mid):
    count, length = kernel.shape[0], kernel.shape[1]
    for at in range(count):
        ground = products(both(own, at), both(far, at))
        tangent = summed(products(both(own_r, at), both(far, at)), products(both(own, at), both(far_r, at)))
        for parity in range(2):
            fields[parity * count + at] = jnp.concatenate([ground[parity], tangent[parity]], 0).astype(bf16)
    for at, even, odd in convolved(fields, blocks, kernel, table, mid):
        yield at, (even[:length], odd[:length]), (even[length:], odd[length:])


def term(partner, partner_r, at, ground, tangent):
    return summed(products(both(partner_r, at), ground), products(both(partner, at), tangent))


def whole(results, length, put):
    area, limit = length * length, (length // 2 + 1) * length
    column = lax.broadcasted_iota(jnp.int32, (length, lane), 1)
    count, stop = slab_count(limit), slab_count(area)
    lowest = stop
    direct, apart = [], []
    for at, parts in enumerate(results):
        direct.append(parts[0] + parts[1])
        apart.append(parts[0] - parts[1])
        if (at + 1) * lane <= limit:
            put(at, direct[at])
        while lowest > limit // lane and needed(lowest - 1, length, limit) <= at:
            lowest -= 1
            there = mirrored(lambda slab: apart[slab], lowest, length, area, limit)
            if lowest < count:
                there = jnp.where(column < limit - lowest * lane, direct[lowest], there)
            put(lowest, there)


def needed(slab, length, limit):
    y = max(slab * lane, limit) // length
    return max((max(slab * lane, limit) + length * length - 2 * length * y + length - 1) // lane, slab if slab * lane < limit else 0)


def store(ref):
    area = ref.shape[1]

    def put(at, value):
        width = min(lane, area - at * lane)
        ref[:, at * lane : at * lane + width] = value[:, :width].astype(ref.dtype)

    return put


def self_body(
    own_in, own_r_in, wide_in, tall_in, kernel_in, blocks_in, mask_in,
    table, near, own, own_r, kernel, blocks, shares, plain,
    mask, wide, tall, plain_r, fields, mid, sems,
):
    length = plain.shape[0]
    half = length // 2 + 1
    count = kernel.shape[0]
    moves = [
        pltpu.make_async_copy(source, target, sems.at[at])
        for at, (source, target) in enumerate(
            [
                (wide_in, wide), (tall_in, tall), (own_in, plain), (own_r_in, plain_r),
                (kernel_in, kernel), (blocks_in, blocks), (mask_in, mask),
            ]
        )
    ]
    for move in moves:
        move.start()
    moves[0].wait()
    moves[1].wait()
    for parity in range(2):
        for at in range(count):
            cols = slice(at * lane, (at + 1) * lane)
            low = tall[:, cols]
            for y in range(0, half, 2):
                rows = [wide[parity, row : row + 1, cols] * low for row in range(y, min(y + 2, half))]
                value = jnp.concatenate(rows, 0)
                table[parity * count + at, y * length : y * length + value.shape[0], :] = value.astype(bf16)
    for move in moves[2:]:
        move.wait()
    for at in range(shares.shape[0]):
        weight = -mixing * mask[0, at].astype(f32)
        shares[at : at + 1, :] = jnp.full((1, shares.shape[1]), weight, f32)
    split(plain, own)
    split(plain_r, own_r)
    for at, ground, tangent in pair(own, own_r, own, own_r, blocks, kernel, table, fields, mid):
        near[at], near[count + at] = term(own, own_r, at, ground, tangent)


def ground_body(own, own_r, plain, blocks, kernel, table, far, cross, ground, carried, fields, mid):
    count = kernel.shape[0]
    split(plain, far)
    for at in range(count):
        for parity, part in enumerate(products(both(own, at), both(far, at))):
            fields[parity * count + at] = part.astype(bf16)
        keep(cross, at, products(both(own_r, at), both(far, at)))
    for at, even, odd in convolved(fields, blocks, kernel, table, mid):
        keep(ground, at, (even, odd))
        keep(carried, at, products(both(own_r, at), (even, odd)))


def far_body(own, own_plain, plain_r, cross, carried, blocks, kernel, table, handed, tangent, fields, mid):
    count, length = kernel.shape[0], kernel.shape[1]
    left, right = natural(own_plain), natural(plain_r)
    kept = {}

    def source(at):
        if at not in kept:
            kept[at] = left(at) * right(at)
        return kept[at]

    for at in range(count):
        for parity, part in enumerate(summed(both(cross, at), halves(source, at, length))):
            fields[parity * count + at] = part.astype(bf16)

    def results():
        for at, even, odd in convolved(fields, blocks, kernel, table, mid):
            keep(tangent, at, (even, odd))
            yield summed(both(carried, at), products(both(own, at), (even, odd)))

    whole(results(), length, store(handed))


def mate_body(
    own, own_r, plain, plain_r, blocks, kernel, table, near, far, far_plain, ground, tangent, shares,
    total, mate, mate_r, far_r, fields, mid,
):
    split(plain, mate)
    split(plain_r, mate_r)
    split(far_plain, far_r)
    first, second, third = (shares[at : at + 1, :lane] for at in range(3))

    def results():
        for at, even, odd in pair(own, own_r, mate, mate_r, blocks, kernel, table, fields, mid):
            prior = term(far, far_r, at, both(ground, at), both(tangent, at))
            parts = zip(both(near, at), term(mate, mate_r, at, even, odd), prior)
            yield tuple(first * a + second * b + third * c for a, b, c in parts)

    whole(results(), plain.shape[0], store(total))


vmem = pl.BlockSpec(memory_space=pltpu.VMEM)
hbm = pl.BlockSpec(memory_space=pltpu.HBM)


def cost(rows, area):
    return pl.CostEstimate(flops=2 * rows * area * area, bytes_accessed=rows * area * 8, transcendentals=0)


def shards(orbitals, response, pair_mask):
    own, own_r = orbitals[0], response[0]
    length, area = own.shape
    folded = (length // 2 + 1) * length
    count = slab_count(folded)
    base = real_table(length)
    wide = np.stack([filled(np.repeat(part, length, axis=1)) for part in half_tables(length)])
    tall = filled(np.tile(base, (1, length // 2 + 1)))
    kernel = filled(coulomb(length)[:, :folded]).reshape(length, count, lane).transpose(1, 0, 2)
    blocks = jnp.asarray(np.kron(np.eye(2), base).astype(np.float32)).astype(bf16)
    far = shifted(own, "blk", 1)
    far_r = shifted(own_r, "blk", 1)
    mate, mate_r = from_partner((own, own_r), "cross", 0)
    plane = lambda kind: jax.ShapeDtypeStruct((length, area), kind)
    parts = jax.ShapeDtypeStruct((2 * count, length, lane), f32)
    held = pltpu.VMEM((2 * count, length, lane), f32)
    inner = [pltpu.VMEM((2 * count, 2 * length, lane), bf16)] * 2
    fixed = lambda value: pltpu.with_memory_space_constraint(jnp.asarray(value), pltpu.HBM)
    table, near, own_parts, own_r_parts, kernel_held, blocks_held, shares, own_plain = pl.pallas_call(
        self_body,
        out_shape=[
            jax.ShapeDtypeStruct((2 * count, folded, lane), bf16), parts, parts, parts,
            jax.ShapeDtypeStruct(kernel.shape, f32), jax.ShapeDtypeStruct(blocks.shape, bf16),
            jax.ShapeDtypeStruct((pair_mask.shape[1], area), f32), plane(bf16),
        ],
        in_specs=[hbm] * 7,
        out_specs=[vmem] * 8,
        scratch_shapes=[
            pltpu.SMEM(pair_mask.shape, jnp.int32), pltpu.VMEM(wide.shape, f32), pltpu.VMEM(tall.shape, f32),
            pltpu.VMEM((length, area), bf16), *inner,
            pltpu.SemaphoreType.DMA((7,)),
        ],
        compiler_params=pltpu.CompilerParams(vmem_limit_bytes=24 << 20),
        cost_estimate=cost(4 * length, area),
    )(*(fixed(value) for value in (own, own_r, wide, tall, kernel, blocks, pair_mask)))
    shared = (blocks_held, kernel_held, table)
    one = [pltpu.VMEM((2 * count, length, lane), bf16)] * 2
    far_parts, cross, ground, carried = pl.pallas_call(
        ground_body,
        out_shape=[parts] * 4,
        in_specs=[vmem] * 6,
        out_specs=[vmem] * 4,
        scratch_shapes=one,
        compiler_params=pltpu.CompilerParams(vmem_limit_bytes=16 << 20),
        cost_estimate=cost(length, area),
    )(own_parts, own_r_parts, far, *shared)
    handed, tangent = pl.pallas_call(
        far_body,
        out_shape=[plane(bf16), parts],
        in_specs=[vmem] * 8,
        out_specs=[vmem] * 2,
        scratch_shapes=one,
        compiler_params=pltpu.CompilerParams(vmem_limit_bytes=16 << 20),
        cost_estimate=cost(length, area),
    )(own_parts, own_plain, far_r, cross, carried, *shared)
    later = shifted(handed, "blk", -1)
    total = pl.pallas_call(
        mate_body,
        out_shape=plane(f32),
        in_specs=[vmem] * 13,
        out_specs=vmem,
        scratch_shapes=[held, held, held, *inner],
        compiler_params=pltpu.CompilerParams(vmem_limit_bytes=16 << 20),
        cost_estimate=cost(2 * length, area),
    )(own_parts, own_r_parts, mate, mate_r, *shared, near, far_parts, far_r, ground, tangent, shares)
    return (total + shares[3:] * later.astype(f32)).astype(bf16)[None]


def solution(mesh):
    spec = P(("grp", "blk", "cross"), None, None)
    return jax.shard_map(
        shards,
        mesh=mesh,
        in_specs=(spec, spec, P(("grp", "blk", "cross"), None)),
        out_specs=spec,
        check_vma=False,
    )
```

```python
import jax
import jax.numpy as jnp
import numpy as np
from jax import lax
from jax.experimental import pallas as pl
from jax.experimental.pallas import tpu as pltpu
from jax.sharding import PartitionSpec as P


mixing = 0.25
lane = 128
bf16 = jnp.bfloat16
f32 = jnp.float32


def from_partner(value, axis, bit):
    mask = 2**bit
    pairs = [(source, source ^ mask) for source in range(lax.axis_size(axis))]
    return lax.ppermute(value, axis, pairs)


def from_side(value, axis, odd):
    devices = lax.axis_size(axis)
    return lax.ppermute(value, axis, [(i, (i + (1 if (i + odd) % 2 == 0 else -1)) % devices) for i in range(devices)])


def real_table(length):
    positions = np.arange(length)
    angles = (positions[:, None] * positions[None, :] % length) * (2.0 * np.pi / length)
    return (np.cos(angles) + np.sin(angles)) / np.sqrt(length)


def half_tables(length):
    half = length // 2 + 1
    positions = np.arange(half)
    angles = (positions[:, None] * positions[None, :] % length) * (2.0 * np.pi / length)
    twice = np.where((positions == 0) | (2 * positions == length), 1.0, 2.0)[:, None]
    return twice * np.cos(angles) / np.sqrt(length), twice * np.sin(angles) * (twice > 1.5) / np.sqrt(length)


def coulomb(length):
    positions = np.arange(length)
    frequency = np.where(positions <= length // 2, positions, positions - length)
    squares = (frequency * frequency).astype(np.float64)
    norm = squares[:, None, None] + squares[None, :, None] + squares[None, None, :]
    values = np.where(norm > 0.5, 1.0 / (0.0625 + 25.0 * norm / (length * length)), 0.0)
    return values.reshape(length, length * length)


def slab_count(width):
    return -(-width // lane)


def filled(values):
    return np.pad(values, ((0, 0), (0, slab_count(values.shape[1]) * lane - values.shape[1]))).astype(np.float32)


def twos(count):
    return [(at, min(2, count - at)) for at in range(0, count, 2)]


def mirrored(source, slab, length, limit, base=0):
    area = length * length
    column = lax.broadcasted_iota(jnp.int32, (length, lane), 1)
    result = None
    at, stop = max(slab * lane, base), min((slab + 1) * lane, limit)
    while at < stop:
        y = at // length
        delta = area - 2 * length * y if y else 0
        origin = (at + delta) // lane
        end = min(stop, (y + 1) * length, (origin + 1) * lane - delta)
        piece = source(origin)
        turn = -delta % lane
        if turn:
            piece = pltpu.roll(piece, turn, 1)
        result = piece if result is None else jnp.where(column >= at - slab * lane, piece, result)
        at = end
    return result


def natural(ref):
    area = ref.shape[1]
    kept = {}

    def slab(at):
        if at not in kept:
            value = ref[:, at * lane : min((at + 1) * lane, area)].astype(f32)
            if value.shape[1] < lane:
                value = jnp.concatenate([value, jnp.zeros((value.shape[0], lane - value.shape[1]), f32)], 1)
            kept[at] = value
        return kept[at]

    return slab


def halves(source, at, length):
    there = mirrored(source, at, length, (length // 2 + 1) * length)
    return 0.5 * (source(at) + there), 0.5 * (source(at) - there)


def split(ref, parts):
    source = natural(ref)
    for at in range(parts.shape[0] // 2):
        keep(parts, at, halves(source, at, ref.shape[0]))


def keep(ref, at, parts):
    count = ref.shape[0] // 2
    ref[at], ref[count + at] = parts


def products(left, right):
    return left[0] * right[0] + left[1] * right[1], left[0] * right[1] + left[1] * right[0]


def both(ref, at):
    count = ref.shape[0] // 2
    return ref[at], ref[count + at]


def summed(left, right):
    return left[0] + right[0], left[1] + right[1]


def through(values, table, spots, firsts):
    count, depth = table.shape[0] // 2, table.shape[1]
    totals = [None] * len(spots)
    for first, size in firsts:
        low, high = first * lane, min((first + size) * lane, depth)
        for which, (parity, at, width) in enumerate(spots):
            base = parity * count
            left = jnp.concatenate([values[base + first + step] for step in range(size)], 1)[:, : high - low]
            right = jnp.concatenate([table[base + at + step, low:high, :] for step in range(width)], 1)
            part = jnp.dot(left, right, preferred_element_type=f32)
            totals[which] = part if totals[which] is None else totals[which] + part
    return totals


def convolved(fields, blocks, kernel, table, mid):
    count, length = kernel.shape[0], kernel.shape[1]
    rows = fields.shape[1]
    tiles = twos(count)
    spots = [[(parity, at, width) for parity in range(2)] for at, width in tiles]
    parts = sum([through(fields, table, spot, tiles) for spot in spots], [])
    step_matrix = blocks[:rows, :rows]
    parts = [jnp.dot(step_matrix, part.astype(bf16), preferred_element_type=f32) for part in parts]
    for which, (parity, at, width) in enumerate(sum(spots, [])):
        gains = jnp.concatenate([kernel[at + step] for step in range(width)], 1)
        parts[which] = (parts[which] * jnp.concatenate([gains] * (rows // length), 0)).astype(bf16)
    parts = [jnp.dot(step_matrix, part, preferred_element_type=f32) for part in parts]
    for (parity, at, width), part in zip(sum(spots, []), parts):
        for step in range(width):
            mid[parity * count + at + step] = part[:, step * lane : (step + 1) * lane].astype(bf16)
    for spot in spots:
        even, odd = through(mid, table, spot, tiles)
        for step in range(spot[0][2]):
            cols = slice(step * lane, (step + 1) * lane)
            yield spot[0][1] + step, even[:, cols], odd[:, cols]


def term(partner, partner_r, at, ground, tangent):
    return summed(products(both(partner_r, at), ground), products(both(partner, at), tangent))


def whole(results, length, put):
    area, limit = length * length, (length // 2 + 1) * length
    column = lax.broadcasted_iota(jnp.int32, (length, lane), 1)
    count, stop = slab_count(limit), slab_count(area)
    lowest = stop
    direct, apart = [], []
    for at, parts in enumerate(results):
        direct.append(parts[0] + parts[1])
        apart.append(parts[0] - parts[1])
        if (at + 1) * lane <= limit:
            put(at, direct[at])
        while lowest > limit // lane and needed(lowest - 1, length, limit) <= at:
            lowest -= 1
            there = mirrored(lambda slab: apart[slab], lowest, length, area, limit)
            if lowest < count:
                there = jnp.where(column < limit - lowest * lane, direct[lowest], there)
            put(lowest, there)


def needed(slab, length, limit):
    y = max(slab * lane, limit) // length
    return max((max(slab * lane, limit) + length * length - 2 * length * y + length - 1) // lane, slab if slab * lane < limit else 0)


def store(ref):
    area = ref.shape[1]

    def put(at, value):
        width = min(lane, area - at * lane)
        ref[:, at * lane : at * lane + width] = value[:, :width].astype(ref.dtype)

    return put


def self_body(
    own_in, own_r_in, wide_in, tall_in, kernel_in, blocks_in, mask_in, mate_in, mate_r_in,
    table, near, own, own_r, kernel, blocks, shares,
    mask, wide, tall, plain, plain_r, mate, mate_r, fields, mid, sems,
):
    length = plain.shape[0]
    half = length // 2 + 1
    count = kernel.shape[0]
    moves = [
        pltpu.make_async_copy(source, target, sems.at[at])
        for at, (source, target) in enumerate(
            [
                (wide_in, wide), (tall_in, tall), (own_in, plain), (own_r_in, plain_r),
                (kernel_in, kernel), (blocks_in, blocks), (mask_in, mask),
            ]
        )
    ]
    for move in moves:
        move.start()
    moves[0].wait()
    moves[1].wait()
    for parity in range(2):
        for at in range(count):
            cols = slice(at * lane, (at + 1) * lane)
            low = tall[:, cols]
            for y in range(0, half, 2):
                rows = [wide[parity, row : row + 1, cols] * low for row in range(y, min(y + 2, half))]
                value = jnp.concatenate(rows, 0)
                table[parity * count + at, y * length : y * length + value.shape[0], :] = value.astype(bf16)
    for move in moves[2:]:
        move.wait()
    even = lax.rem(lax.axis_index("blk"), 2) == 0
    prior, later = mask[0, 2].astype(f32), mask[0, 3].astype(f32)
    weights = (
        mask[0, 0].astype(f32), mask[0, 1].astype(f32),
        jnp.where(even, later, prior), jnp.where(even, prior, later),
    )
    for at in range(shares.shape[0]):
        weight = -mixing * weights[at]
        shares[at : at + 1, :] = jnp.full((1, shares.shape[1]), weight, f32)
    split(plain, own)
    split(plain_r, own_r)
    split(mate_in, mate)
    split(mate_r_in, mate_r)
    for at in range(count):
        rows = both_fields(own, own_r, own, own_r, at), both_fields(own, own_r, mate, mate_r, at)
        fill(fields, at, [field for pair in rows for field in pair])
    first, second = shares[0:1, :lane], shares[1:2, :lane]
    for at, even, odd in convolved(fields, blocks, kernel, table, mid):
        fieldwise = [(even[row * length : (row + 1) * length], odd[row * length : (row + 1) * length]) for row in range(4)]
        parts = zip(term(own, own_r, at, *fieldwise[:2]), term(mate, mate_r, at, *fieldwise[2:]))
        keep(near, at, tuple(first * a + second * b for a, b in parts))


def both_fields(own, own_r, far, far_r, at):
    tangent = summed(products(both(own_r, at), both(far, at)), products(both(own, at), both(far_r, at)))
    return products(both(own, at), both(far, at)), tangent


def fill(fields, at, rows):
    count = fields.shape[0] // 2
    for parity in range(2):
        fields[parity * count + at] = jnp.concatenate([row[parity] for row in rows], 0).astype(bf16)


def early_body(
    own, own_r, side_plain, far_plain, blocks, kernel, table,
    side, far, side_cross, far_cross, side_ground, far_ground, fields, mid,
):
    count, length = kernel.shape[0], kernel.shape[1]
    split(side_plain, side)
    split(far_plain, far)
    for at in range(count):
        fill(fields, at, [products(both(own, at), both(side, at)), products(both(own, at), both(far, at))])
        keep(side_cross, at, products(both(own_r, at), both(side, at)))
        keep(far_cross, at, products(both(own_r, at), both(far, at)))
    for at, even, odd in convolved(fields, blocks, kernel, table, mid):
        keep(side_ground, at, (even[:length], odd[:length]))
        keep(far_ground, at, (even[length:], odd[length:]))


def last_body(
    own, side_plain, far_plain, side, far, side_cross, far_cross, side_ground, far_ground, before, shares,
    blocks, kernel, table,
    out, side_r, far_r, summed_up, staged, fields, mid, sem,
):
    count, length = kernel.shape[0], kernel.shape[1]
    third, fourth = shares[2:3, :lane], shares[3:4, :lane]
    split(side_plain, side_r)
    split(far_plain, far_r)
    for at in range(count):
        rows = ((side_cross, side_r), (far_cross, far_r))
        fill(fields, at, [summed(both(cross, at), products(both(own, at), both(far_one, at))) for cross, far_one in rows])
    for at in range(count):
        parts = zip(both(before, at), products(both(side_r, at), both(side_ground, at)), products(both(far_r, at), both(far_ground, at)))
        keep(summed_up, at, tuple(a + third * b + fourth * c for a, b, c in parts))

    def results():
        for at, even, odd in convolved(fields, blocks, kernel, table, mid):
            near_part = products(both(side, at), (even[:length], odd[:length]))
            far_part = products(both(far, at), (even[length:], odd[length:]))
            yield tuple(a + third * b + fourth * c for a, b, c in zip(both(summed_up, at), near_part, far_part))

    whole(results(), length, store(staged))
    move = pltpu.make_async_copy(staged, out, sem)
    move.start()
    move.wait()


vmem = pl.BlockSpec(memory_space=pltpu.VMEM)
hbm = pl.BlockSpec(memory_space=pltpu.HBM)


def cost(rows, area):
    return pl.CostEstimate(flops=2 * rows * area * area, bytes_accessed=rows * area * 8, transcendentals=0)


def shards(orbitals, response, pair_mask):
    own, own_r = orbitals[0], response[0]
    length, area = own.shape
    folded = (length // 2 + 1) * length
    count = slab_count(folded)
    base = real_table(length)
    wide = np.stack([filled(np.repeat(part, length, axis=1)) for part in half_tables(length)])
    tall = filled(np.tile(base, (1, length // 2 + 1)))
    kernel = filled(coulomb(length)[:, :folded]).reshape(length, count, lane).transpose(1, 0, 2)
    blocks = jnp.asarray(np.kron(np.eye(4), base).astype(np.float32)).astype(bf16)

    side = from_side(own, "blk", 0)
    side_r = from_side(own_r, "blk", 0)
    mate = from_partner(own, "cross", 0)
    mate_r = from_partner(own_r, "cross", 0)
    plane = lambda kind: jax.ShapeDtypeStruct((length, area), kind)
    parts = jax.ShapeDtypeStruct((2 * count, length, lane), f32)
    held = pltpu.VMEM((2 * count, length, lane), f32)
    room = lambda rows: [pltpu.VMEM((2 * count, rows * length, lane), bf16)] * 2
    fixed = lambda value: pltpu.with_memory_space_constraint(jnp.asarray(value), pltpu.HBM)
    params = pltpu.CompilerParams(vmem_limit_bytes=20 << 20)
    first = pl.pallas_call(
        self_body,
        out_shape=[
            jax.ShapeDtypeStruct((2 * count, folded, lane), bf16), parts, parts, parts,
            jax.ShapeDtypeStruct(kernel.shape, f32), jax.ShapeDtypeStruct(blocks.shape, bf16),
            jax.ShapeDtypeStruct((pair_mask.shape[1], area), f32),
        ],
        in_specs=[hbm] * 7 + [vmem] * 2,
        out_specs=[vmem] * 7,
        scratch_shapes=[
            pltpu.SMEM(pair_mask.shape, jnp.int32), pltpu.VMEM(wide.shape, f32), pltpu.VMEM(tall.shape, f32),
            pltpu.VMEM((length, area), bf16), pltpu.VMEM((length, area), bf16), held, held, *room(4),
            pltpu.SemaphoreType.DMA((7,)),
        ],
        compiler_params=pltpu.CompilerParams(vmem_limit_bytes=24 << 20),
        cost_estimate=cost(6 * length, area),
    )
    table, near, own_parts, own_r_parts, kernel_held, blocks_held, shares = first(
        *(fixed(value) for value in (own, own_r, wide, tall, kernel, blocks, pair_mask)), mate, mate_r
    )
    far = from_side(own, "blk", 1)
    far_r = from_side(own_r, "blk", 1)
    shared = (blocks_held, kernel_held, table)
    early = pl.pallas_call(
        early_body,
        out_shape=[parts] * 6,
        in_specs=[vmem] * 7,
        out_specs=[vmem] * 6,
        scratch_shapes=room(2),
        compiler_params=params,
        cost_estimate=cost(2 * length, area),
    )
    known = early(own_parts, own_r_parts, side, far, *shared)
    out = pl.pallas_call(
        last_body,
        out_shape=plane(bf16),
        in_specs=[vmem] * 14,
        out_specs=hbm,
        scratch_shapes=[held, held, held, pltpu.VMEM((length, area), bf16), *room(2), pltpu.SemaphoreType.DMA],
        compiler_params=params,
        cost_estimate=cost(2 * length, area),
    )(own_parts, side_r, far_r, *known, near, shares, *shared)
    return out[None]


def solution(mesh):
    spec = P(("grp", "blk", "cross"), None, None)
    return jax.shard_map(
        shards,
        mesh=mesh,
        in_specs=(spec, spec, P(("grp", "blk", "cross"), None)),
        out_specs=spec,
        check_vma=False,
    )
```

```python
import jax
import jax.numpy as jnp
import numpy as np
from jax import lax
from jax.experimental import pallas as pl
from jax.experimental.pallas import tpu as pltpu
from jax.sharding import PartitionSpec as P


mixing = 0.25
lane = 128
bf16 = jnp.bfloat16
f32 = jnp.float32


def from_partner(value, axis, bit):
    mask = 2**bit
    pairs = [(source, source ^ mask) for source in range(lax.axis_size(axis))]
    return lax.ppermute(value, axis, pairs)


def from_side(value, axis, odd):
    devices = lax.axis_size(axis)
    return lax.ppermute(value, axis, [(i, (i + (1 if (i + odd) % 2 == 0 else -1)) % devices) for i in range(devices)])


def real_table(length):
    positions = np.arange(length)
    angles = (positions[:, None] * positions[None, :] % length) * (2.0 * np.pi / length)
    return (np.cos(angles) + np.sin(angles)) / np.sqrt(length)


def half_tables(length):
    half = length // 2 + 1
    positions = np.arange(half)
    angles = (positions[:, None] * positions[None, :] % length) * (2.0 * np.pi / length)
    twice = np.where((positions == 0) | (2 * positions == length), 1.0, 2.0)[:, None]
    return twice * np.cos(angles) / np.sqrt(length), twice * np.sin(angles) * (twice > 1.5) / np.sqrt(length)


def coulomb(length):
    positions = np.arange(length)
    frequency = np.where(positions <= length // 2, positions, positions - length)
    squares = (frequency * frequency).astype(np.float64)
    norm = squares[:, None, None] + squares[None, :, None] + squares[None, None, :]
    values = np.where(norm > 0.5, 1.0 / (0.0625 + 25.0 * norm / (length * length)), 0.0)
    return values.reshape(length, length * length)


def slab_count(width):
    return -(-width // lane)


def filled(values):
    return np.pad(values, ((0, 0), (0, slab_count(values.shape[1]) * lane - values.shape[1]))).astype(np.float32)


def twos(count):
    return [(at, min(2, count - at)) for at in range(0, count, 2)]


def mirrored(source, slab, length, limit, base=0):
    area = length * length
    column = lax.broadcasted_iota(jnp.int32, (length, lane), 1)
    result = None
    at, stop = max(slab * lane, base), min((slab + 1) * lane, limit)
    while at < stop:
        y = at // length
        delta = area - 2 * length * y if y else 0
        origin = (at + delta) // lane
        end = min(stop, (y + 1) * length, (origin + 1) * lane - delta)
        piece = source(origin)
        turn = -delta % lane
        if turn:
            piece = pltpu.roll(piece, turn, 1)
        result = piece if result is None else jnp.where(column >= at - slab * lane, piece, result)
        at = end
    return result


def natural(ref):
    area = ref.shape[1]
    kept = {}

    def slab(at):
        if at not in kept:
            value = ref[:, at * lane : min((at + 1) * lane, area)].astype(f32)
            if value.shape[1] < lane:
                value = jnp.concatenate([value, jnp.zeros((value.shape[0], lane - value.shape[1]), f32)], 1)
            kept[at] = value
        return kept[at]

    return slab


def halves(source, at, length):
    there = mirrored(source, at, length, (length // 2 + 1) * length)
    return 0.5 * (source(at) + there), 0.5 * (source(at) - there)


def split(ref, parts):
    source = natural(ref)
    for at in range(parts.shape[0] // 2):
        keep(parts, at, halves(source, at, ref.shape[0]))


def keep(ref, at, parts):
    count = ref.shape[0] // 2
    ref[at], ref[count + at] = parts


def products(left, right):
    return left[0] * right[0] + left[1] * right[1], left[0] * right[1] + left[1] * right[0]


def both(ref, at):
    count = ref.shape[0] // 2
    return ref[at], ref[count + at]


def summed(left, right):
    return left[0] + right[0], left[1] + right[1]


def through(values, table, spots, firsts):
    count, depth = table.shape[0] // 2, table.shape[1]
    totals = [None] * len(spots)
    for first, size in firsts:
        low, high = first * lane, min((first + size) * lane, depth)
        for which, (parity, at, width) in enumerate(spots):
            base = parity * count
            left = jnp.concatenate([values[base + first + step] for step in range(size)], 1)[:, : high - low]
            right = jnp.concatenate([table[base + at + step, low:high, :] for step in range(width)], 1)
            part = jnp.dot(left, right, preferred_element_type=f32)
            totals[which] = part if totals[which] is None else totals[which] + part
    return totals


def convolved(fields, blocks, kernel, table, mid):
    count, length = kernel.shape[0], kernel.shape[1]
    rows = fields.shape[1]
    tiles = twos(count)
    spots = [[(parity, at, width) for parity in range(2)] for at, width in tiles]
    parts = sum([through(fields, table, spot, tiles) for spot in spots], [])
    step_matrix = blocks[:rows, :rows]
    parts = [jnp.dot(step_matrix, part.astype(bf16), preferred_element_type=f32) for part in parts]
    for which, (parity, at, width) in enumerate(sum(spots, [])):
        gains = jnp.concatenate([kernel[at + step] for step in range(width)], 1)
        parts[which] = (parts[which] * jnp.concatenate([gains] * (rows // length), 0)).astype(bf16)
    parts = [jnp.dot(step_matrix, part, preferred_element_type=f32) for part in parts]
    for (parity, at, width), part in zip(sum(spots, []), parts):
        for step in range(width):
            mid[parity * count + at + step] = part[:, step * lane : (step + 1) * lane].astype(bf16)
    for spot in spots:
        even, odd = through(mid, table, spot, tiles)
        for step in range(spot[0][2]):
            cols = slice(step * lane, (step + 1) * lane)
            yield spot[0][1] + step, even[:, cols], odd[:, cols]


def term(partner, partner_r, at, ground, tangent):
    return summed(products(both(partner_r, at), ground), products(both(partner, at), tangent))


def whole(results, length, put):
    area, limit = length * length, (length // 2 + 1) * length
    column = lax.broadcasted_iota(jnp.int32, (length, lane), 1)
    count, stop = slab_count(limit), slab_count(area)
    lowest = stop
    direct, apart = [], []
    for at, parts in enumerate(results):
        direct.append(parts[0] + parts[1])
        apart.append(parts[0] - parts[1])
        if (at + 1) * lane <= limit:
            put(at, direct[at])
        while lowest > limit // lane and needed(lowest - 1, length, limit) <= at:
            lowest -= 1
            there = mirrored(lambda slab: apart[slab], lowest, length, area, limit)
            if lowest < count:
                there = jnp.where(column < limit - lowest * lane, direct[lowest], there)
            put(lowest, there)


def needed(slab, length, limit):
    y = max(slab * lane, limit) // length
    return max((max(slab * lane, limit) + length * length - 2 * length * y + length - 1) // lane, slab if slab * lane < limit else 0)


def store(ref):
    area = ref.shape[1]

    def put(at, value):
        width = min(lane, area - at * lane)
        ref[:, at * lane : at * lane + width] = value[:, :width].astype(ref.dtype)

    return put


def self_body(
    own_in, own_r_in, wide_in, tall_in, kernel_in, blocks_in, mask_in,
    table, near, own, own_r, kernel, blocks, shares,
    mask, wide, tall, plain, plain_r, fields, mid, sems,
):
    length = plain.shape[0]
    half = length // 2 + 1
    count = kernel.shape[0]
    moves = [
        pltpu.make_async_copy(source, target, sems.at[at])
        for at, (source, target) in enumerate(
            [
                (wide_in, wide), (tall_in, tall), (own_in, plain), (own_r_in, plain_r),
                (kernel_in, kernel), (blocks_in, blocks), (mask_in, mask),
            ]
        )
    ]
    for move in moves:
        move.start()
    moves[0].wait()
    moves[1].wait()
    for parity in range(2):
        for at in range(count):
            cols = slice(at * lane, (at + 1) * lane)
            low = tall[:, cols]
            for y in range(0, half, 2):
                rows = [wide[parity, row : row + 1, cols] * low for row in range(y, min(y + 2, half))]
                value = jnp.concatenate(rows, 0)
                table[parity * count + at, y * length : y * length + value.shape[0], :] = value.astype(bf16)
    for move in moves[2:]:
        move.wait()
    even = lax.rem(lax.axis_index("blk"), 2) == 0
    prior, later = mask[0, 2].astype(f32), mask[0, 3].astype(f32)
    weights = (
        mask[0, 0].astype(f32), mask[0, 1].astype(f32),
        jnp.where(even, later, prior), jnp.where(even, prior, later),
    )
    for at in range(shares.shape[0]):
        weight = -mixing * weights[at]
        shares[at : at + 1, :] = jnp.full((1, shares.shape[1]), weight, f32)
    split(plain, own)
    split(plain_r, own_r)
    for at in range(count):
        fill(fields, at, both_fields(own, own_r, own, own_r, at))
    for at, even, odd in convolved(fields, blocks, kernel, table, mid):
        part = term(own, own_r, at, (even[:length], odd[:length]), (even[length:], odd[length:]))
        keep(near, at, tuple(shares[0:1, :lane] * value for value in part))


def both_fields(own, own_r, far, far_r, at):
    tangent = summed(products(both(own_r, at), both(far, at)), products(both(own, at), both(far_r, at)))
    return products(both(own, at), both(far, at)), tangent


def fill(fields, at, rows):
    count = fields.shape[0] // 2
    for parity in range(2):
        fields[parity * count + at] = jnp.concatenate([row[parity] for row in rows], 0).astype(bf16)


def early_body(
    own, own_r, side_plain, far_plain, mate_plain, mate_r_plain, near, shares, blocks, kernel, table,
    side, far, side_cross, far_cross, side_ground, far_ground, total, mate, mate_r, fields, mid,
):
    count, length = kernel.shape[0], kernel.shape[1]
    for plain, parts in ((mate_plain, mate), (mate_r_plain, mate_r), (side_plain, side), (far_plain, far)):
        split(plain, parts)
    for at in range(count):
        grounds = products(both(own, at), both(side, at)), products(both(own, at), both(far, at))
        fill(fields, at, [*grounds, *both_fields(own, own_r, mate, mate_r, at)])
        keep(side_cross, at, products(both(own_r, at), both(side, at)))
        keep(far_cross, at, products(both(own_r, at), both(far, at)))
    for at, even, odd in convolved(fields, blocks, kernel, table, mid):
        fieldwise = [(even[row * length : (row + 1) * length], odd[row * length : (row + 1) * length]) for row in range(4)]
        keep(side_ground, at, fieldwise[0])
        keep(far_ground, at, fieldwise[1])
        parts = zip(both(near, at), term(mate, mate_r, at, *fieldwise[2:]))
        keep(total, at, tuple(a + shares[1:2, :lane] * b for a, b in parts))


def last_body(
    own, side_plain, far_plain, side, far, side_cross, far_cross, side_ground, far_ground, before, shares,
    blocks, kernel, table,
    out, side_r, far_r, summed_up, staged, fields, mid, sem,
):
    count, length = kernel.shape[0], kernel.shape[1]
    third, fourth = shares[2:3, :lane], shares[3:4, :lane]
    split(side_plain, side_r)
    split(far_plain, far_r)
    for at in range(count):
        rows = ((side_cross, side_r), (far_cross, far_r))
        fill(fields, at, [summed(both(cross, at), products(both(own, at), both(far_one, at))) for cross, far_one in rows])
    for at in range(count):
        parts = zip(both(before, at), products(both(side_r, at), both(side_ground, at)), products(both(far_r, at), both(far_ground, at)))
        keep(summed_up, at, tuple(a + third * b + fourth * c for a, b, c in parts))

    def results():
        for at, even, odd in convolved(fields, blocks, kernel, table, mid):
            near_part = products(both(side, at), (even[:length], odd[:length]))
            far_part = products(both(far, at), (even[length:], odd[length:]))
            yield tuple(a + third * b + fourth * c for a, b, c in zip(both(summed_up, at), near_part, far_part))

    whole(results(), length, store(staged))
    move = pltpu.make_async_copy(staged, out, sem)
    move.start()
    move.wait()


vmem = pl.BlockSpec(memory_space=pltpu.VMEM)
hbm = pl.BlockSpec(memory_space=pltpu.HBM)


def cost(rows, area):
    return pl.CostEstimate(flops=2 * rows * area * area, bytes_accessed=rows * area * 8, transcendentals=0)


def shards(orbitals, response, pair_mask):
    own, own_r = orbitals[0], response[0]
    length, area = own.shape
    folded = (length // 2 + 1) * length
    count = slab_count(folded)
    base = real_table(length)
    wide = np.stack([filled(np.repeat(part, length, axis=1)) for part in half_tables(length)])
    tall = filled(np.tile(base, (1, length // 2 + 1)))
    kernel = filled(coulomb(length)[:, :folded]).reshape(length, count, lane).transpose(1, 0, 2)
    blocks = jnp.asarray(np.kron(np.eye(4), base).astype(np.float32)).astype(bf16)

    side = from_side(own, "blk", 0)
    side_r = from_side(own_r, "blk", 0)
    mate = from_partner(own, "cross", 0)
    mate_r = from_partner(own_r, "cross", 0)
    plane = lambda kind: jax.ShapeDtypeStruct((length, area), kind)
    parts = jax.ShapeDtypeStruct((2 * count, length, lane), f32)
    held = pltpu.VMEM((2 * count, length, lane), f32)
    room = lambda rows: [pltpu.VMEM((2 * count, rows * length, lane), bf16)] * 2
    fixed = lambda value: pltpu.with_memory_space_constraint(jnp.asarray(value), pltpu.HBM)
    params = pltpu.CompilerParams(vmem_limit_bytes=20 << 20)
    first = pl.pallas_call(
        self_body,
        out_shape=[
            jax.ShapeDtypeStruct((2 * count, folded, lane), bf16), parts, parts, parts,
            jax.ShapeDtypeStruct(kernel.shape, f32), jax.ShapeDtypeStruct(blocks.shape, bf16),
            jax.ShapeDtypeStruct((pair_mask.shape[1], area), f32),
        ],
        in_specs=[hbm] * 7,
        out_specs=[vmem] * 7,
        scratch_shapes=[
            pltpu.SMEM(pair_mask.shape, jnp.int32), pltpu.VMEM(wide.shape, f32), pltpu.VMEM(tall.shape, f32),
            pltpu.VMEM((length, area), bf16), pltpu.VMEM((length, area), bf16), *room(2),
            pltpu.SemaphoreType.DMA((7,)),
        ],
        compiler_params=pltpu.CompilerParams(vmem_limit_bytes=24 << 20),
        cost_estimate=cost(4 * length, area),
    )
    table, near, own_parts, own_r_parts, kernel_held, blocks_held, shares = first(
        *(fixed(value) for value in (own, own_r, wide, tall, kernel, blocks, pair_mask))
    )
    far = from_side(own, "blk", 1)
    far_r = from_side(own_r, "blk", 1)
    shared = (blocks_held, kernel_held, table)
    early = pl.pallas_call(
        early_body,
        out_shape=[parts] * 7,
        in_specs=[vmem] * 11,
        out_specs=[vmem] * 7,
        scratch_shapes=[held, held, *room(4)],
        compiler_params=params,
        cost_estimate=cost(4 * length, area),
    )
    known = early(own_parts, own_r_parts, side, far, mate, mate_r, near, shares, *shared)
    out = pl.pallas_call(
        last_body,
        out_shape=plane(bf16),
        in_specs=[vmem] * 14,
        out_specs=hbm,
        scratch_shapes=[held, held, held, pltpu.VMEM((length, area), bf16), *room(2), pltpu.SemaphoreType.DMA],
        compiler_params=params,
        cost_estimate=cost(2 * length, area),
    )(own_parts, side_r, far_r, *known, shares, *shared)
    return out[None]


def solution(mesh):
    spec = P(("grp", "blk", "cross"), None, None)
    return jax.shard_map(
        shards,
        mesh=mesh,
        in_specs=(spec, spec, P(("grp", "blk", "cross"), None)),
        out_specs=spec,
        check_vma=False,
    )
```

```python
import jax
import jax.numpy as jnp
import numpy as np
from jax import lax
from jax.experimental import pallas as pl
from jax.experimental.pallas import tpu as pltpu
from jax.sharding import PartitionSpec as P


mixing = 0.25
lane = 128
bf16 = jnp.bfloat16
f32 = jnp.float32


def from_partner(value, axis, bit):
    mask = 2**bit
    pairs = [(source, source ^ mask) for source in range(lax.axis_size(axis))]
    return lax.ppermute(value, axis, pairs)


def from_side(value, axis, odd):
    devices = lax.axis_size(axis)
    return lax.ppermute(value, axis, [(i, (i + (1 if (i + odd) % 2 == 0 else -1)) % devices) for i in range(devices)])


def real_table(length):
    positions = np.arange(length)
    angles = (positions[:, None] * positions[None, :] % length) * (2.0 * np.pi / length)
    return (np.cos(angles) + np.sin(angles)) / np.sqrt(length)


def half_tables(length):
    half = length // 2 + 1
    positions = np.arange(half)
    angles = (positions[:, None] * positions[None, :] % length) * (2.0 * np.pi / length)
    twice = np.where((positions == 0) | (2 * positions == length), 1.0, 2.0)[:, None]
    return twice * np.cos(angles) / np.sqrt(length), twice * np.sin(angles) * (twice > 1.5) / np.sqrt(length)


def coulomb(length):
    positions = np.arange(length)
    frequency = np.where(positions <= length // 2, positions, positions - length)
    squares = (frequency * frequency).astype(np.float64)
    norm = squares[:, None, None] + squares[None, :, None] + squares[None, None, :]
    values = np.where(norm > 0.5, 1.0 / (0.0625 + 25.0 * norm / (length * length)), 0.0)
    return values.reshape(length, length * length)


def slab_count(width):
    return -(-width // lane)


def filled(values):
    return np.pad(values, ((0, 0), (0, slab_count(values.shape[1]) * lane - values.shape[1]))).astype(np.float32)


def twos(count):
    return [(at, min(2, count - at)) for at in range(0, count, 2)]


def mirrored(source, slab, length, limit, base=0):
    area = length * length
    column = lax.broadcasted_iota(jnp.int32, (length, lane), 1)
    result = None
    at, stop = max(slab * lane, base), min((slab + 1) * lane, limit)
    while at < stop:
        y = at // length
        delta = area - 2 * length * y if y else 0
        origin = (at + delta) // lane
        end = min(stop, (y + 1) * length, (origin + 1) * lane - delta)
        piece = source(origin)
        turn = -delta % lane
        if turn:
            piece = pltpu.roll(piece, turn, 1)
        result = piece if result is None else jnp.where(column >= at - slab * lane, piece, result)
        at = end
    return result


def natural(ref):
    area = ref.shape[1]
    kept = {}

    def slab(at):
        if at not in kept:
            value = ref[:, at * lane : min((at + 1) * lane, area)].astype(f32)
            if value.shape[1] < lane:
                value = jnp.concatenate([value, jnp.zeros((value.shape[0], lane - value.shape[1]), f32)], 1)
            kept[at] = value
        return kept[at]

    return slab


def halves(source, at, length):
    there = mirrored(source, at, length, (length // 2 + 1) * length)
    return 0.5 * (source(at) + there), 0.5 * (source(at) - there)


def split(ref, parts):
    source = natural(ref)
    for at in range(parts.shape[0] // 2):
        keep(parts, at, halves(source, at, ref.shape[0]))


def keep(ref, at, parts):
    count = ref.shape[0] // 2
    ref[at], ref[count + at] = parts


def products(left, right):
    return left[0] * right[0] + left[1] * right[1], left[0] * right[1] + left[1] * right[0]


def both(ref, at):
    count = ref.shape[0] // 2
    return ref[at], ref[count + at]


def summed(left, right):
    return left[0] + right[0], left[1] + right[1]


def through(values, table, spots, firsts):
    count, depth = table.shape[0] // 2, table.shape[1]
    totals = [None] * len(spots)
    for first, size in firsts:
        low, high = first * lane, min((first + size) * lane, depth)
        for which, (parity, at, width) in enumerate(spots):
            base = parity * count
            left = jnp.concatenate([values[base + first + step] for step in range(size)], 1)[:, : high - low]
            right = jnp.concatenate([table[base + at + step, low:high, :] for step in range(width)], 1)
            part = jnp.dot(left, right, preferred_element_type=f32)
            totals[which] = part if totals[which] is None else totals[which] + part
    return totals


def convolved(fields, blocks, kernel, table, mid):
    count, length = kernel.shape[0], kernel.shape[1]
    rows = fields.shape[1]
    tiles = twos(count)
    spots = [[(parity, at, width) for parity in range(2)] for at, width in tiles]
    parts = sum([through(fields, table, spot, tiles) for spot in spots], [])
    step_matrix = blocks[:rows, :rows]
    parts = [jnp.dot(step_matrix, part.astype(bf16), preferred_element_type=f32) for part in parts]
    for which, (parity, at, width) in enumerate(sum(spots, [])):
        gains = jnp.concatenate([kernel[at + step] for step in range(width)], 1)
        parts[which] = (parts[which] * jnp.concatenate([gains] * (rows // length), 0)).astype(bf16)
    parts = [jnp.dot(step_matrix, part, preferred_element_type=f32) for part in parts]
    for (parity, at, width), part in zip(sum(spots, []), parts):
        for step in range(width):
            mid[parity * count + at + step] = part[:, step * lane : (step + 1) * lane].astype(bf16)
    for spot in spots:
        even, odd = through(mid, table, spot, tiles)
        for step in range(spot[0][2]):
            cols = slice(step * lane, (step + 1) * lane)
            yield spot[0][1] + step, even[:, cols], odd[:, cols]


def term(partner, partner_r, at, ground, tangent):
    return summed(products(both(partner_r, at), ground), products(both(partner, at), tangent))


def whole(results, length, put):
    area, limit = length * length, (length // 2 + 1) * length
    column = lax.broadcasted_iota(jnp.int32, (length, lane), 1)
    count, stop = slab_count(limit), slab_count(area)
    lowest = stop
    direct, apart = [], []
    for at, parts in enumerate(results):
        direct.append(parts[0] + parts[1])
        apart.append(parts[0] - parts[1])
        if (at + 1) * lane <= limit:
            put(at, direct[at])
        while lowest > limit // lane and needed(lowest - 1, length, limit) <= at:
            lowest -= 1
            there = mirrored(lambda slab: apart[slab], lowest, length, area, limit)
            if lowest < count:
                there = jnp.where(column < limit - lowest * lane, direct[lowest], there)
            put(lowest, there)


def needed(slab, length, limit):
    y = max(slab * lane, limit) // length
    return max((max(slab * lane, limit) + length * length - 2 * length * y + length - 1) // lane, slab if slab * lane < limit else 0)


def store(ref):
    area = ref.shape[1]

    def put(at, value):
        width = min(lane, area - at * lane)
        ref[:, at * lane : at * lane + width] = value[:, :width].astype(ref.dtype)

    return put


def self_body(
    own_in, own_r_in, wide_in, tall_in, kernel_in, blocks_in, mask_in,
    table, near, own, own_r, kernel, blocks, shares,
    mask, wide, tall, plain, plain_r, fields, mid, sems,
):
    length = plain.shape[0]
    half = length // 2 + 1
    count = kernel.shape[0]
    moves = [
        pltpu.make_async_copy(source, target, sems.at[at])
        for at, (source, target) in enumerate(
            [
                (wide_in, wide), (tall_in, tall), (own_in, plain), (own_r_in, plain_r),
                (kernel_in, kernel), (blocks_in, blocks), (mask_in, mask),
            ]
        )
    ]
    for move in moves:
        move.start()
    moves[0].wait()
    moves[1].wait()
    for parity in range(2):
        for at in range(count):
            cols = slice(at * lane, (at + 1) * lane)
            low = tall[:, cols]
            for y in range(0, half, 2):
                rows = [wide[parity, row : row + 1, cols] * low for row in range(y, min(y + 2, half))]
                value = jnp.concatenate(rows, 0)
                table[parity * count + at, y * length : y * length + value.shape[0], :] = value.astype(bf16)
    for move in moves[2:]:
        move.wait()
    even = lax.rem(lax.axis_index("blk"), 2) == 0
    prior, later = mask[0, 2].astype(f32), mask[0, 3].astype(f32)
    weights = (
        mask[0, 0].astype(f32), mask[0, 1].astype(f32),
        jnp.where(even, later, prior), jnp.where(even, prior, later),
    )
    for at in range(shares.shape[0]):
        weight = -mixing * weights[at]
        shares[at : at + 1, :] = jnp.full((1, shares.shape[1]), weight, f32)
    split(plain, own)
    split(plain_r, own_r)
    for at in range(count):
        fill(fields, at, both_fields(own, own_r, own, own_r, at))
    for at, even, odd in convolved(fields, blocks, kernel, table, mid):
        part = term(own, own_r, at, (even[:length], odd[:length]), (even[length:], odd[length:]))
        keep(near, at, tuple(shares[0:1, :lane] * value for value in part))


def both_fields(own, own_r, far, far_r, at):
    tangent = summed(products(both(own_r, at), both(far, at)), products(both(own, at), both(far_r, at)))
    return products(both(own, at), both(far, at)), tangent


def fill(fields, at, rows):
    count = fields.shape[0] // 2
    for parity in range(2):
        fields[parity * count + at] = jnp.concatenate([row[parity] for row in rows], 0).astype(bf16)


def early_body(
    own, own_r, side_plain, far_plain, mate_plain, mate_r_plain, near, shares, blocks, kernel, table,
    side, far, side_cross, far_cross, side_ground, far_ground, total, mate, mate_r, fields, mid,
):
    count, length = kernel.shape[0], kernel.shape[1]
    for plain, parts in ((mate_plain, mate), (mate_r_plain, mate_r), (side_plain, side), (far_plain, far)):
        split(plain, parts)
    for at in range(count):
        grounds = products(both(own, at), both(side, at)), products(both(own, at), both(far, at))
        fill(fields, at, [*grounds, *both_fields(own, own_r, mate, mate_r, at)])
        keep(side_cross, at, products(both(own_r, at), both(side, at)))
        keep(far_cross, at, products(both(own_r, at), both(far, at)))
    for at, even, odd in convolved(fields, blocks, kernel, table, mid):
        fieldwise = [(even[row * length : (row + 1) * length], odd[row * length : (row + 1) * length]) for row in range(4)]
        keep(side_ground, at, fieldwise[0])
        keep(far_ground, at, fieldwise[1])
        parts = zip(both(near, at), term(mate, mate_r, at, *fieldwise[2:]))
        keep(total, at, tuple(a + shares[1:2, :lane] * b for a, b in parts))


def side_body(own, plain, cross, ground, before, shares, field, total):
    source = natural(plain)
    for at in range(field.shape[0] // 2):
        part = halves(source, at, plain.shape[0])
        keep(field, at, summed(both(cross, at), products(both(own, at), part)))
        share = shares[2:3, :lane]
        keep(total, at, tuple(a + share * b for a, b in zip(both(before, at), products(part, both(ground, at)))))


def last_body(
    own, far_plain, side_field, side, far, far_cross, far_ground, before, shares, blocks, kernel, table,
    out, far_r, summed_up, staged, fields, mid, sem,
):
    count, length = kernel.shape[0], kernel.shape[1]
    third, fourth = shares[2:3, :lane], shares[3:4, :lane]
    split(far_plain, far_r)
    for at in range(count):
        fill(fields, at, [both(side_field, at), summed(both(far_cross, at), products(both(own, at), both(far_r, at)))])
    for at in range(count):
        parts = zip(both(before, at), products(both(far_r, at), both(far_ground, at)))
        keep(summed_up, at, tuple(a + fourth * b for a, b in parts))

    def results():
        for at, even, odd in convolved(fields, blocks, kernel, table, mid):
            near_part = products(both(side, at), (even[:length], odd[:length]))
            far_part = products(both(far, at), (even[length:], odd[length:]))
            yield tuple(a + third * b + fourth * c for a, b, c in zip(both(summed_up, at), near_part, far_part))

    whole(results(), length, store(staged))
    move = pltpu.make_async_copy(staged, out, sem)
    move.start()
    move.wait()


vmem = pl.BlockSpec(memory_space=pltpu.VMEM)
hbm = pl.BlockSpec(memory_space=pltpu.HBM)


def cost(rows, area):
    return pl.CostEstimate(flops=2 * rows * area * area, bytes_accessed=rows * area * 8, transcendentals=0)


def shards(orbitals, response, pair_mask):
    own, own_r = orbitals[0], response[0]
    length, area = own.shape
    folded = (length // 2 + 1) * length
    count = slab_count(folded)
    base = real_table(length)
    wide = np.stack([filled(np.repeat(part, length, axis=1)) for part in half_tables(length)])
    tall = filled(np.tile(base, (1, length // 2 + 1)))
    kernel = filled(coulomb(length)[:, :folded]).reshape(length, count, lane).transpose(1, 0, 2)
    blocks = jnp.asarray(np.kron(np.eye(4), base).astype(np.float32)).astype(bf16)

    side = from_side(own, "blk", 0)
    side_r = from_side(own_r, "blk", 0)
    mate = from_partner(own, "cross", 0)
    mate_r = from_partner(own_r, "cross", 0)
    plane = lambda kind: jax.ShapeDtypeStruct((length, area), kind)
    parts = jax.ShapeDtypeStruct((2 * count, length, lane), f32)
    held = pltpu.VMEM((2 * count, length, lane), f32)
    room = lambda rows: [pltpu.VMEM((2 * count, rows * length, lane), bf16)] * 2
    fixed = lambda value: pltpu.with_memory_space_constraint(jnp.asarray(value), pltpu.HBM)
    params = pltpu.CompilerParams(vmem_limit_bytes=20 << 20)
    first = pl.pallas_call(
        self_body,
        out_shape=[
            jax.ShapeDtypeStruct((2 * count, folded, lane), bf16), parts, parts, parts,
            jax.ShapeDtypeStruct(kernel.shape, f32), jax.ShapeDtypeStruct(blocks.shape, bf16),
            jax.ShapeDtypeStruct((pair_mask.shape[1], area), f32),
        ],
        in_specs=[hbm] * 7,
        out_specs=[vmem] * 7,
        scratch_shapes=[
            pltpu.SMEM(pair_mask.shape, jnp.int32), pltpu.VMEM(wide.shape, f32), pltpu.VMEM(tall.shape, f32),
            pltpu.VMEM((length, area), bf16), pltpu.VMEM((length, area), bf16), *room(2),
            pltpu.SemaphoreType.DMA((7,)),
        ],
        compiler_params=pltpu.CompilerParams(vmem_limit_bytes=24 << 20),
        cost_estimate=cost(4 * length, area),
    )
    table, near, own_parts, own_r_parts, kernel_held, blocks_held, shares = first(
        *(fixed(value) for value in (own, own_r, wide, tall, kernel, blocks, pair_mask))
    )
    far = from_side(own, "blk", 1)
    far_r = from_side(own_r, "blk", 1)
    shared = (blocks_held, kernel_held, table)
    early = pl.pallas_call(
        early_body,
        out_shape=[parts] * 7,
        in_specs=[vmem] * 11,
        out_specs=[vmem] * 7,
        scratch_shapes=[held, held, *room(4)],
        compiler_params=params,
        cost_estimate=cost(4 * length, area),
    )
    side_parts, far_parts, side_cross, far_cross, side_ground, far_ground, total = early(own_parts, own_r_parts, side, far, mate, mate_r, near, shares, *shared)
    tangent = pl.pallas_call(
        side_body,
        out_shape=[parts] * 2,
        in_specs=[vmem] * 6,
        out_specs=[vmem] * 2,
        compiler_params=params,
        cost_estimate=cost(2, area),
    )
    side_field, total = tangent(own_parts, side_r, side_cross, side_ground, total, shares)
    out = pl.pallas_call(
        last_body,
        out_shape=plane(bf16),
        in_specs=[vmem] * 12,
        out_specs=hbm,
        scratch_shapes=[held, held, pltpu.VMEM((length, area), bf16), *room(2), pltpu.SemaphoreType.DMA],
        compiler_params=params,
        cost_estimate=cost(2 * length, area),
    )(own_parts, far_r, side_field, side_parts, far_parts, far_cross, far_ground, total, shares, *shared)
    return out[None]


def solution(mesh):
    spec = P(("grp", "blk", "cross"), None, None)
    return jax.shard_map(
        shards,
        mesh=mesh,
        in_specs=(spec, spec, P(("grp", "blk", "cross"), None)),
        out_specs=spec,
        check_vma=False,
    )
```

```python
import jax
import jax.numpy as jnp
import numpy as np
from jax import lax
from jax.experimental import pallas as pl
from jax.experimental.pallas import tpu as pltpu
from jax.sharding import PartitionSpec as P


mixing = 0.25
lane = 128
bf16 = jnp.bfloat16
f32 = jnp.float32


def from_partner(value, axis, bit):
    mask = 2**bit
    pairs = [(source, source ^ mask) for source in range(lax.axis_size(axis))]
    return lax.ppermute(value, axis, pairs)


def from_side(value, axis, odd):
    devices = lax.axis_size(axis)
    return lax.ppermute(value, axis, [(i, (i + (1 if (i + odd) % 2 == 0 else -1)) % devices) for i in range(devices)])


def real_table(length):
    positions = np.arange(length)
    angles = (positions[:, None] * positions[None, :] % length) * (2.0 * np.pi / length)
    return (np.cos(angles) + np.sin(angles)) / np.sqrt(length)


def half_tables(length):
    half = length // 2 + 1
    positions = np.arange(half)
    angles = (positions[:, None] * positions[None, :] % length) * (2.0 * np.pi / length)
    twice = np.where((positions == 0) | (2 * positions == length), 1.0, 2.0)[:, None]
    return twice * np.cos(angles) / np.sqrt(length), twice * np.sin(angles) * (twice > 1.5) / np.sqrt(length)


def coulomb(length):
    positions = np.arange(length)
    frequency = np.where(positions <= length // 2, positions, positions - length)
    squares = (frequency * frequency).astype(np.float64)
    norm = squares[:, None, None] + squares[None, :, None] + squares[None, None, :]
    values = np.where(norm > 0.5, 1.0 / (0.0625 + 25.0 * norm / (length * length)), 0.0)
    return values.reshape(length, length * length)


def slab_count(width):
    return -(-width // lane)


def filled(values):
    return np.pad(values, ((0, 0), (0, slab_count(values.shape[1]) * lane - values.shape[1]))).astype(np.float32)


def twos(count):
    return [(at, min(2, count - at)) for at in range(0, count, 2)]


def mirrored(source, slab, length, limit, base=0):
    area = length * length
    column = lax.broadcasted_iota(jnp.int32, (length, lane), 1)
    result = None
    at, stop = max(slab * lane, base), min((slab + 1) * lane, limit)
    while at < stop:
        y = at // length
        delta = area - 2 * length * y if y else 0
        origin = (at + delta) // lane
        end = min(stop, (y + 1) * length, (origin + 1) * lane - delta)
        piece = source(origin)
        turn = -delta % lane
        if turn:
            piece = pltpu.roll(piece, turn, 1)
        result = piece if result is None else jnp.where(column >= at - slab * lane, piece, result)
        at = end
    return result


def natural(ref):
    area = ref.shape[1]
    kept = {}

    def slab(at):
        if at not in kept:
            value = ref[:, at * lane : min((at + 1) * lane, area)].astype(f32)
            if value.shape[1] < lane:
                value = jnp.concatenate([value, jnp.zeros((value.shape[0], lane - value.shape[1]), f32)], 1)
            kept[at] = value
        return kept[at]

    return slab


def halves(source, at, length):
    there = mirrored(source, at, length, (length // 2 + 1) * length)
    return 0.5 * (source(at) + there), 0.5 * (source(at) - there)


def split(ref, parts):
    source = natural(ref)
    for at in range(parts.shape[0] // 2):
        keep(parts, at, halves(source, at, ref.shape[0]))


def keep(ref, at, parts):
    count = ref.shape[0] // 2
    ref[at], ref[count + at] = parts


def products(left, right):
    return left[0] * right[0] + left[1] * right[1], left[0] * right[1] + left[1] * right[0]


def both(ref, at):
    count = ref.shape[0] // 2
    return ref[at], ref[count + at]


def summed(left, right):
    return left[0] + right[0], left[1] + right[1]


def through(values, table, spots, firsts):
    count, depth = table.shape[0] // 2, table.shape[1]
    totals = [None] * len(spots)
    for first, size in firsts:
        low, high = first * lane, min((first + size) * lane, depth)
        for which, (parity, at, width) in enumerate(spots):
            base = parity * count
            left = jnp.concatenate([values[base + first + step] for step in range(size)], 1)[:, : high - low]
            right = jnp.concatenate([table[base + at + step, low:high, :] for step in range(width)], 1)
            part = jnp.dot(left, right, preferred_element_type=f32)
            totals[which] = part if totals[which] is None else totals[which] + part
    return totals


def convolved(fields, blocks, kernel, table, mid):
    count, length = kernel.shape[0], kernel.shape[1]
    rows = fields.shape[1]
    tiles = twos(count)
    spots = [[(parity, at, width) for parity in range(2)] for at, width in tiles]
    parts = sum([through(fields, table, spot, tiles) for spot in spots], [])
    step_matrix = blocks[:rows, :rows]
    parts = [jnp.dot(step_matrix, part.astype(bf16), preferred_element_type=f32) for part in parts]
    for which, (parity, at, width) in enumerate(sum(spots, [])):
        gains = jnp.concatenate([kernel[at + step] for step in range(width)], 1)
        parts[which] = (parts[which] * jnp.concatenate([gains] * (rows // length), 0)).astype(bf16)
    parts = [jnp.dot(step_matrix, part, preferred_element_type=f32) for part in parts]
    for (parity, at, width), part in zip(sum(spots, []), parts):
        for step in range(width):
            mid[parity * count + at + step] = part[:, step * lane : (step + 1) * lane].astype(bf16)
    for spot in spots:
        even, odd = through(mid, table, spot, tiles)
        for step in range(spot[0][2]):
            cols = slice(step * lane, (step + 1) * lane)
            yield spot[0][1] + step, even[:, cols], odd[:, cols]


def term(partner, partner_r, at, ground, tangent):
    return summed(products(both(partner_r, at), ground), products(both(partner, at), tangent))


def whole(results, length, put):
    area, limit = length * length, (length // 2 + 1) * length
    column = lax.broadcasted_iota(jnp.int32, (length, lane), 1)
    count, stop = slab_count(limit), slab_count(area)
    lowest = stop
    direct, apart = [], []
    for at, parts in enumerate(results):
        direct.append(parts[0] + parts[1])
        apart.append(parts[0] - parts[1])
        if (at + 1) * lane <= limit:
            put(at, direct[at])
        while lowest > limit // lane and needed(lowest - 1, length, limit) <= at:
            lowest -= 1
            there = mirrored(lambda slab: apart[slab], lowest, length, area, limit)
            if lowest < count:
                there = jnp.where(column < limit - lowest * lane, direct[lowest], there)
            put(lowest, there)


def needed(slab, length, limit):
    y = max(slab * lane, limit) // length
    return max((max(slab * lane, limit) + length * length - 2 * length * y + length - 1) // lane, slab if slab * lane < limit else 0)


def store(ref):
    area = ref.shape[1]

    def put(at, value):
        width = min(lane, area - at * lane)
        ref[:, at * lane : at * lane + width] = value[:, :width].astype(ref.dtype)

    return put


def self_body(
    own_in, own_r_in, wide_in, tall_in, kernel_in, blocks_in, mask_in,
    table, near, own, own_r, kernel, blocks, shares,
    mask, wide, tall, plain, plain_r, fields, mid, sems,
):
    length = plain.shape[0]
    half = length // 2 + 1
    count = kernel.shape[0]
    moves = [
        pltpu.make_async_copy(source, target, sems.at[at])
        for at, (source, target) in enumerate(
            [
                (wide_in, wide), (tall_in, tall), (own_in, plain), (own_r_in, plain_r),
                (kernel_in, kernel), (blocks_in, blocks), (mask_in, mask),
            ]
        )
    ]
    for move in moves:
        move.start()
    moves[0].wait()
    moves[1].wait()
    for parity in range(2):
        for at in range(count):
            cols = slice(at * lane, (at + 1) * lane)
            low = tall[:, cols]
            for y in range(0, half, 2):
                rows = [wide[parity, row : row + 1, cols] * low for row in range(y, min(y + 2, half))]
                value = jnp.concatenate(rows, 0)
                table[parity * count + at, y * length : y * length + value.shape[0], :] = value.astype(bf16)
    for move in moves[2:]:
        move.wait()
    even = lax.rem(lax.axis_index("blk"), 2) == 0
    prior, later = mask[0, 2].astype(f32), mask[0, 3].astype(f32)
    weights = (
        mask[0, 0].astype(f32), mask[0, 1].astype(f32),
        jnp.where(even, later, prior), jnp.where(even, prior, later),
    )
    for at in range(shares.shape[0]):
        weight = -mixing * weights[at]
        shares[at : at + 1, :] = jnp.full((1, shares.shape[1]), weight, f32)
    split(plain, own)
    split(plain_r, own_r)
    for at in range(count):
        fill(fields, at, both_fields(own, own_r, own, own_r, at))
    for at, even, odd in convolved(fields, blocks, kernel, table, mid):
        part = term(own, own_r, at, (even[:length], odd[:length]), (even[length:], odd[length:]))
        keep(near, at, tuple(shares[0:1, :lane] * value for value in part))


def both_fields(own, own_r, far, far_r, at):
    tangent = summed(products(both(own_r, at), both(far, at)), products(both(own, at), both(far_r, at)))
    return products(both(own, at), both(far, at)), tangent


def fill(fields, at, rows):
    count = fields.shape[0] // 2
    for parity in range(2):
        fields[parity * count + at] = jnp.concatenate([row[parity] for row in rows], 0).astype(bf16)


def early_body(
    own, own_r, side_plain, far_plain, mate_plain, mate_r_plain, near, shares, blocks, kernel, table,
    side, far, side_cross, far_cross, side_ground, far_ground, total, mate, mate_r, fields, mid,
):
    count, length = kernel.shape[0], kernel.shape[1]
    for plain, parts in ((mate_plain, mate), (mate_r_plain, mate_r), (side_plain, side), (far_plain, far)):
        split(plain, parts)
    for at in range(count):
        grounds = products(both(own, at), both(side, at)), products(both(own, at), both(far, at))
        fill(fields, at, [*grounds, *both_fields(own, own_r, mate, mate_r, at)])
        keep(side_cross, at, products(both(own_r, at), both(side, at)))
        keep(far_cross, at, products(both(own_r, at), both(far, at)))
    for at, even, odd in convolved(fields, blocks, kernel, table, mid):
        fieldwise = [(even[row * length : (row + 1) * length], odd[row * length : (row + 1) * length]) for row in range(4)]
        keep(side_ground, at, fieldwise[0])
        keep(far_ground, at, fieldwise[1])
        parts = zip(both(near, at), term(mate, mate_r, at, *fieldwise[2:]))
        keep(total, at, tuple(a + shares[1:2, :lane] * b for a, b in parts))


def side_body(own, plain, cross, ground, before, shares, field, total):
    source = natural(plain)
    for at in range(field.shape[0] // 2):
        part = halves(source, at, plain.shape[0])
        keep(field, at, summed(both(cross, at), products(both(own, at), part)))
        share = shares[2:3, :lane]
        keep(total, at, tuple(a + share * b for a, b in zip(both(before, at), products(part, both(ground, at)))))


def last_body(
    own, far_plain, side_field, side, far, far_cross, far_ground, before, shares, blocks, kernel, table,
    out, far_r, summed_up, staged, fields, mid, sem,
):
    count, length = kernel.shape[0], kernel.shape[1]
    third, fourth = shares[2:3, :lane], shares[3:4, :lane]
    split(far_plain, far_r)
    for at in range(count):
        fill(fields, at, [both(side_field, at), summed(both(far_cross, at), products(both(own, at), both(far_r, at)))])
    for at in range(count):
        parts = zip(both(before, at), products(both(far_r, at), both(far_ground, at)))
        keep(summed_up, at, tuple(a + fourth * b for a, b in parts))

    def results():
        for at, even, odd in convolved(fields, blocks, kernel, table, mid):
            near_part = products(both(side, at), (even[:length], odd[:length]))
            far_part = products(both(far, at), (even[length:], odd[length:]))
            yield tuple(a + third * b + fourth * c for a, b, c in zip(both(summed_up, at), near_part, far_part))

    slabs = slab_count(out.shape[1])
    edges = (0, count // 2 * lane, slabs // 4 * 3 * lane, out.shape[1])
    spans = [slice(low, high) for low, high in zip(edges, edges[1:])]
    moves = [pltpu.make_async_copy(staged.at[:, span], out.at[:, span], sem.at[at]) for at, span in enumerate(spans)]
    missing = [{at for at in range(slabs) if span.start <= at * lane < span.stop} for span in spans]
    simple = store(staged)

    def put(at, value):
        simple(at, value)
        for group, move in zip(missing, moves):
            if at in group:
                group.remove(at)
                if not group:
                    move.start()

    whole(results(), length, put)
    for move in moves:
        move.wait()


vmem = pl.BlockSpec(memory_space=pltpu.VMEM)
hbm = pl.BlockSpec(memory_space=pltpu.HBM)


def cost(rows, area):
    return pl.CostEstimate(flops=2 * rows * area * area, bytes_accessed=rows * area * 8, transcendentals=0)


def shards(orbitals, response, pair_mask):
    own, own_r = orbitals[0], response[0]
    length, area = own.shape
    folded = (length // 2 + 1) * length
    count = slab_count(folded)
    base = real_table(length)
    wide = np.stack([filled(np.repeat(part, length, axis=1)) for part in half_tables(length)])
    tall = filled(np.tile(base, (1, length // 2 + 1)))
    kernel = filled(coulomb(length)[:, :folded]).reshape(length, count, lane).transpose(1, 0, 2)
    blocks = jnp.asarray(np.kron(np.eye(4), base).astype(np.float32)).astype(bf16)

    side = from_side(own, "blk", 0)
    side_r = from_side(own_r, "blk", 0)
    mate = from_partner(own, "cross", 0)
    mate_r = from_partner(own_r, "cross", 0)
    plane = lambda kind: jax.ShapeDtypeStruct((length, area), kind)
    parts = jax.ShapeDtypeStruct((2 * count, length, lane), f32)
    held = pltpu.VMEM((2 * count, length, lane), f32)
    room = lambda rows: [pltpu.VMEM((2 * count, rows * length, lane), bf16)] * 2
    fixed = lambda value: pltpu.with_memory_space_constraint(jnp.asarray(value), pltpu.HBM)
    params = pltpu.CompilerParams(vmem_limit_bytes=20 << 20)
    first = pl.pallas_call(
        self_body,
        out_shape=[
            jax.ShapeDtypeStruct((2 * count, folded, lane), bf16), parts, parts, parts,
            jax.ShapeDtypeStruct(kernel.shape, f32), jax.ShapeDtypeStruct(blocks.shape, bf16),
            jax.ShapeDtypeStruct((pair_mask.shape[1], area), f32),
        ],
        in_specs=[hbm] * 7,
        out_specs=[vmem] * 7,
        scratch_shapes=[
            pltpu.SMEM(pair_mask.shape, jnp.int32), pltpu.VMEM(wide.shape, f32), pltpu.VMEM(tall.shape, f32),
            pltpu.VMEM((length, area), bf16), pltpu.VMEM((length, area), bf16), *room(2),
            pltpu.SemaphoreType.DMA((7,)),
        ],
        compiler_params=pltpu.CompilerParams(vmem_limit_bytes=24 << 20),
        cost_estimate=cost(4 * length, area),
    )
    table, near, own_parts, own_r_parts, kernel_held, blocks_held, shares = first(
        *(fixed(value) for value in (own, own_r, wide, tall, kernel, blocks, pair_mask))
    )
    far = from_side(own, "blk", 1)
    far_r = from_side(own_r, "blk", 1)
    shared = (blocks_held, kernel_held, table)
    early = pl.pallas_call(
        early_body,
        out_shape=[parts] * 7,
        in_specs=[vmem] * 11,
        out_specs=[vmem] * 7,
        scratch_shapes=[held, held, *room(4)],
        compiler_params=params,
        cost_estimate=cost(4 * length, area),
    )
    side_parts, far_parts, side_cross, far_cross, side_ground, far_ground, total = early(own_parts, own_r_parts, side, far, mate, mate_r, near, shares, *shared)
    tangent = pl.pallas_call(
        side_body,
        out_shape=[parts] * 2,
        in_specs=[vmem] * 6,
        out_specs=[vmem] * 2,
        compiler_params=params,
        cost_estimate=cost(2, area),
    )
    side_field, total = tangent(own_parts, side_r, side_cross, side_ground, total, shares)
    out = pl.pallas_call(
        last_body,
        out_shape=plane(bf16),
        in_specs=[vmem] * 12,
        out_specs=hbm,
        scratch_shapes=[held, held, pltpu.VMEM((length, area), bf16), *room(2), pltpu.SemaphoreType.DMA((3,))],
        compiler_params=params,
        cost_estimate=cost(2 * length, area),
    )(own_parts, far_r, side_field, side_parts, far_parts, far_cross, far_ground, total, shares, *shared)
    return out[None]


def solution(mesh):
    spec = P(("grp", "blk", "cross"), None, None)
    return jax.shard_map(
        shards,
        mesh=mesh,
        in_specs=(spec, spec, P(("grp", "blk", "cross"), None)),
        out_specs=spec,
        check_vma=False,
    )
```
